32 devices in a mesh: section: 2 (over core), blk: 4 (over z), shard: 4 (over y, x).
Axes of the slice: x: 2, y: 2, z: 4, core: 2. Of those that a mesh axis runs over, the one named last changes fastest.
Arguments:
- ids: int32 [2, 4, 1024], P(None, 'shard', 'blk'), may hold values from 0 to 31999
- targets: int32 [2, 4, 1024, 2], P(None, 'shard', 'blk'), may hold values from 0 to 31999
- segments: int32 [2, 4, 1024], P(None, 'shard'), may hold values from 0 to 3, never falling along the last dimension, each value on 1 to 512 neighbouring positions
- table: float32 [32000, 768], P(('section', 'blk', 'shard')), may hold values from -0.4375 to 0.4375
- table_m: float32 [32000, 768], P(('section', 'blk', 'shard')), may hold values from -9.536743e-06 to 9.536743e-06
- table_v: float32 [32000, 768], P(('section', 'blk', 'shard')), may hold values from 2e-12 to 2e-11
- blocks: float32 [2, 1728, 64, 64], P('section', ('blk', 'shard')), may hold values from -1.1547005 to 1.1547005
- left_stats: float32 [2, 1728, 64, 64], P('section', ('blk', 'shard')), may hold values from -1.6e-07 to 2e-06, as said below
- right_stats: float32 [2, 1728, 64, 64], P('section', ('blk', 'shard')), may hold values from -1.6e-07 to 2e-06, as said below
- left_root: float32 [2, 1728, 64, 64], P('section', ('blk', 'shard')), may hold values from -24 to 180, as said below
- right_root: float32 [2, 1728, 64, 64], P('section', ('blk', 'shard')), may hold values from -24 to 180, as said below
- gains: float32 [5, 768], replicated, may hold values from 0.5 to 1.5
- gains_m: float32 [5, 768], replicated, may hold values from -0.00061035156 to 0.00061035156
- gains_v: float32 [5, 768], replicated, may hold values from 1e-10 to 1e-09
Outputs:
- loss: float32 [], replicated
- clip_norm: float32 [], replicated
- table_new: float32 [32000, 768], P(('section', 'blk', 'shard'))
- table_m_new: float32 [32000, 768], P(('section', 'blk', 'shard'))
- table_v_new: float32 [32000, 768], P(('section', 'blk', 'shard'))
- table_low: bfloat16 [32000, 768], P(('section', 'blk', 'shard'))
- blocks_new: float32 [2, 1728, 64, 64], P('section', ('blk', 'shard'))
- blocks_low: bfloat16 [2, 1728, 64, 64], P('section', ('blk', 'shard'))
- left_new: float32 [2, 1728, 64, 64], P('section', ('blk', 'shard'))
- right_new: float32 [2, 1728, 64, 64], P('section', ('blk', 'shard'))
- gains_new: float32 [5, 768], replicated
- gains_m_new: float32 [5, 768], replicated
- gains_v_new: float32 [5, 768], replicated
The draws below stay inside these ranges and needn't reach their ends.
Inputs may be any that keep to these rules, and one draw needn't show every extreme that they name: `left_stats`: symmetric. `right_stats`: symmetric. `left_root`: symmetric. `right_root`: symmetric.
All inputs are finite; a program needn't handle non-finite values.
Results may differ from the reference program's by a relative error of at most 0.014.
Values may be sent and summed in bfloat16 or wider, within the bound.
A program may use at most 448 MiB of HBM per device.

```python
import math
import jax
import jax.numpy as jnp
import numpy as np
from jax import lax

D = 768
HEADS = 12
HEAD_DIM = 64
FF = 2048
VOCAB = 32000
BS = 64
DOCS = 4
MICRO = 2
SECTIONS = 2
SEQS = 4
SEQ_LEN = 1024
NBLOCKS = 1728


def symmetric_draw(key, diag_lo, diag_hi, off_scale):
    first_key, second_key = jax.random.split(key)
    shape_all = (SECTIONS, NBLOCKS, BS, BS)
    noise_draw = jax.random.truncated_normal(first_key, -4.0, 4.0, shape_all, jnp.float32)
    noise_draw = (noise_draw + jnp.swapaxes(noise_draw, -1, -2)) * 0.5 * off_scale
    diagonal = jnp.exp(jax.random.uniform(second_key, (SECTIONS, NBLOCKS, BS), jnp.float32, jnp.log(diag_lo), jnp.log(diag_hi)))
    identity = (jnp.arange(BS)[:, None] == jnp.arange(BS)[None, :]).astype(jnp.float32)
    return noise_draw * (1.0 - identity) + diagonal[..., None] * identity


def draw_blocks(key, part):
    noise_draw = jax.random.truncated_normal(key, -4.0, 4.0, (SECTIONS, NBLOCKS, BS, BS), jnp.float32)
    block_index = jnp.arange(NBLOCKS)
    count_qkv = D // BS * (3 * D // BS)
    count_out = D // BS * (D // BS)
    count_gate = D // BS * (2 * FF // BS)
    block_scale = jnp.where(block_index < count_qkv, D ** (-0.5), jnp.where(block_index < count_qkv + count_out, 8.0 * D ** (-0.5), jnp.where(block_index < count_qkv + count_out + count_gate, D ** (-0.5), FF ** (-0.5))))
    return noise_draw * block_scale[None, :, None, None].astype(jnp.float32)


def draw_left_stats(key, part):
    return symmetric_draw(jax.random.fold_in(key, 11), 5e-07, 2e-06, 4e-08)


def draw_right_stats(key, part):
    return symmetric_draw(jax.random.fold_in(key, 12), 5e-07, 2e-06, 4e-08)


def draw_left_root(key, part):
    return symmetric_draw(jax.random.fold_in(key, 13), 60.0, 180.0, 6.0)


def draw_right_root(key, part):
    return symmetric_draw(jax.random.fold_in(key, 14), 60.0, 180.0, 6.0)


def place_ends(array, key, low, high):
    longest = array.shape.index(max(array.shape))
    spots = []
    for shift in (0, 1):
        where = [jax.random.randint(jax.random.fold_in(key, axis), (), 0, length) for axis, length in enumerate(array.shape)]
        where[longest] = (where[longest] + shift) % array.shape[longest]
        spots.append(tuple(where))
    return array.at[spots[0]].set(low).at[spots[1]].set(high)


def shard_levels(stream_key, shape, cuts, low, top_value):
    gain, own = 1.0, jax.random.fold_in(stream_key, 6)
    for position, blocks in cuts:
        steps = jnp.exp(jax.random.uniform(jax.random.fold_in(own, position), (blocks,), jnp.float32, low / len(cuts), top_value / len(cuts)))
        gain = gain * jnp.repeat(steps, shape[position] // blocks).reshape([-1 if axis == position else 1 for axis in range(len(shape))])
    return gain


def profile(count, total, most, slope):
    weights = [(1 << 20) // math.isqrt(grade ** slope) + 1 for grade in range(2, count + 1)]
    surplus, counts = total - most - (count - 1), [1] * (count - 1)
    while surplus > 0:
        candidates = [i for i in range(count - 1) if counts[i] < most]
        pool, budget = sum([weights[i] for i in candidates]), surplus
        for i in candidates:
            more = min(most - counts[i], max(1, budget * weights[i] // pool), surplus)
            counts[i] = counts[i] + more
            surplus = surplus - more
    return np.array([most] + counts)


def ragged_sizes(stream_key, number_of, total, most, skew):
    if number_of == 2:
        one = jax.random.randint(stream_key, (), max(1, total - most), min(most, total - 1) + 1)
        return jnp.stack([one, total - one])
    sizes = jnp.asarray(profile(number_of, total, most, skew), jnp.int32)
    couples = (number_of - 1) // 2
    source_of, receiver = sizes[1:1 + 2 * couples:2], sizes[2:2 + 2 * couples:2]
    margin = jnp.minimum(source_of - 1, most - receiver)
    passed = jax.random.randint(jax.random.fold_in(stream_key, 1), (couples,), 0, 1 << 20) % (margin + 1)
    sizes = sizes.at[1:1 + 2 * couples:2].set(source_of - passed).at[2:2 + 2 * couples:2].set(receiver + passed)
    return sizes[jax.random.permutation(jax.random.fold_in(stream_key, 2), number_of)]


def bell_draw(own_key, extent, deviation, bound, cuts=(), kind=jnp.bfloat16):
    level = shard_levels(own_key, extent, cuts, -0.22, 0.18) if cuts else 1.0
    result = jax.random.normal(own_key, extent, jnp.float32) * deviation * level
    return jnp.minimum(jnp.maximum(result, -bound), bound).astype(kind)


def setup_inputs(seed: int = 0) -> dict:
    splits = jax.random.split(jax.random.key(seed), 15)
    return {
        "ids": place_ends(jax.random.randint(splits[0], (MICRO, SEQS, SEQ_LEN), 0, VOCAB), jax.random.fold_in(splits[0], 1), 0, VOCAB - 1).astype(jnp.int32),
        "targets": place_ends(jax.random.randint(splits[1], (MICRO, SEQS, SEQ_LEN, 2), 0, VOCAB), jax.random.fold_in(splits[1], 1), 0, VOCAB - 1).astype(jnp.int32),
        "segments": jax.vmap(lambda own: jnp.searchsorted(jnp.cumsum(ragged_sizes(own, DOCS, SEQ_LEN, SEQ_LEN // 2, 2)), jnp.arange(SEQ_LEN), side="right"))(jax.random.split(splits[2], MICRO * SEQS)).reshape((MICRO, SEQS, SEQ_LEN)).astype(jnp.int32),
        "table": bell_draw(splits[3], (VOCAB, D), 0.07, 0.4375, ((0, 32),), jnp.float32),
        "table_m": bell_draw(splits[4], (VOCAB, D), (1.5e-6), 9.5367431640625e-06, ((0, 32),), jnp.float32),
        "table_v": jnp.clip(jnp.exp(math.log(1.9999999920083944e-11) - 2.3025851 * jax.random.uniform(splits[5], (VOCAB, D), jnp.float32) ** shard_levels(splits[5], (VOCAB, D), ((0, 32),), -0.2, 0.2)), 1.9999999920083944e-12, 1.9999999920083944e-11),
        "blocks": draw_blocks(jax.random.fold_in(splits[14], 71), 0),
        "left_stats": draw_left_stats(jax.random.fold_in(splits[14], 71), 0),
        "right_stats": draw_right_stats(jax.random.fold_in(splits[14], 71), 0),
        "left_root": draw_left_root(jax.random.fold_in(splits[14], 71), 0),
        "right_root": draw_right_root(jax.random.fold_in(splits[14], 71), 0),
        "gains": jnp.clip(1.0 + 0.1 * jax.random.normal(splits[11], (2 * SECTIONS + 1, D), jnp.float32), 0.5, 1.5),
        "gains_m": bell_draw(splits[12], (2 * SECTIONS + 1, D), (1e-4), 0.00061035156, (), jnp.float32),
        "gains_v": jnp.clip(jnp.exp(jax.random.uniform(splits[13], (2 * SECTIONS + 1, D), jnp.float32, math.log(1.000000013351432e-10), math.log(9.999999717180685e-10))), 1.000000013351432e-10, 9.999999717180685e-10),
    }


@jax.custom_vjp
def low(v):
    return lax.optimization_barrier(v.astype(jnp.bfloat16)).astype(jnp.float32)

@jax.custom_vjp
def low_back(v):
    return v

def low_keep(v):
    return (low(v), None)

def low_pass(kept, grad):
    return (grad,)

def back_keep(v):
    return (v, None)

def back_low(kept, grad):
    return (low(grad),)
low.defvjp(low_keep, low_pass)
low_back.defvjp(back_keep, back_low)
norm_eps = 1e-05
rope_base = 10000.0
clip_bound = 0.08
shampoo_rate = 0.1
adam_rate = 0.02
beta_first = 0.9
beta_second = 0.95
adam_eps = 1e-08
weight_decay = 0.1
stat_decay = 0.5
second_weight = 0.3
highest = lax.Precision.HIGHEST

def product(left_side, right_side):
    return jnp.dot(left_side, right_side, precision=highest, preferred_element_type=jnp.float32)

def matrix_layout():
    return ((D, 3 * D), (D, D), (D, 2 * FF), (FF, D))

def assemble(pieces):
    matrices = []
    offset = 0
    for row_count, col_count in matrix_layout():
        row_blocks = row_count // BS
        col_blocks = col_count // BS
        chosen = pieces[offset:offset + row_blocks * col_blocks].reshape(row_blocks, col_blocks, BS, BS)
        matrices.append(chosen.transpose(0, 2, 1, 3).reshape(row_count, col_count))
        offset += row_blocks * col_blocks
    return matrices

def rms_scale(states, gain_row):
    return states * lax.rsqrt(lax.optimization_barrier(jnp.mean(states * states, axis=-1, keepdims=True)) + norm_eps) * gain_row

def rope_tables(positions):
    half_dim = HEAD_DIM // 2
    frequency = rope_base ** (-jnp.arange(half_dim, dtype=jnp.float32) * 2.0 / HEAD_DIM)
    angles = positions.astype(jnp.float32)[:, None] * frequency[None, :]
    cosine = jnp.concatenate([jnp.cos(angles), jnp.cos(angles)], axis=-1)[:, None, :]
    sine_table = jnp.concatenate([jnp.sin(angles), jnp.sin(angles)], axis=-1)[:, None, :]
    return (cosine, sine_table)

def rotate(values, cosine, sine_table):
    half_dim = HEAD_DIM // 2
    turned = jnp.concatenate([-values[..., half_dim:], values[..., :half_dim]], axis=-1)
    return values * cosine + turned * sine_table

def attend(queries, key_heads, value_heads, segment_row):
    query_rows = min(512, SEQ_LEN)
    key_pos = jnp.arange(SEQ_LEN, dtype=jnp.int32)
    scale_factor = HEAD_DIM ** (-0.5)

    def one_block(block_index):
        first_row = (block_index * query_rows).astype(jnp.int32)
        query_block = lax.dynamic_slice_in_dim(queries, first_row, query_rows, 0)
        query_pos = first_row + jnp.arange(query_rows, dtype=jnp.int32)
        query_seg = lax.dynamic_slice_in_dim(segment_row, first_row, query_rows, 0)
        scores = low_back(jnp.einsum('qhe,khe->hqk', query_block, key_heads, precision=highest) * scale_factor)
        allowed = (key_pos[None, :] <= query_pos[:, None]) & (segment_row[None, :] == query_seg[:, None])
        exp_scores = jnp.where(allowed[None], jnp.exp(scores), 0.0)
        totals = lax.optimization_barrier(jnp.sum(exp_scores, axis=-1))
        weighted = low_back(jnp.einsum('hqk,khe->qhe', low(exp_scores), value_heads, precision=highest))
        return low(weighted / totals.T[:, :, None])
    outputs = lax.map(jax.checkpoint(one_block), jnp.arange(SEQ_LEN // query_rows, dtype=jnp.int32))
    return outputs.reshape(SEQ_LEN, D)

def decoder_layer(states, matrices, gain_first, gain_second, segment_row):
    w_qkv, w_out, w_gate_up, w_down = matrices
    normed = low(rms_scale(states, gain_first))
    projected = low_back(product(normed, w_qkv))
    cosine, sine_table = rope_tables(jnp.arange(SEQ_LEN, dtype=jnp.int32))
    queries = low(rotate(projected[:, :D].reshape(SEQ_LEN, HEADS, HEAD_DIM), cosine, sine_table))
    key_heads = low(rotate(projected[:, D:2 * D].reshape(SEQ_LEN, HEADS, HEAD_DIM), cosine, sine_table))
    value_heads = low(projected[:, 2 * D:].reshape(SEQ_LEN, HEADS, HEAD_DIM))
    attended = attend(queries, key_heads, value_heads, segment_row)
    mid_state = states + low_back(product(attended, w_out))
    normed_mid = low(rms_scale(mid_state, gain_second))
    gate_up = low_back(product(normed_mid, w_gate_up))
    hidden = low(jax.nn.silu(gate_up[:, :FF]) * gate_up[:, FF:])
    return mid_state + low_back(product(hidden, w_down))

def sequence_loss(table_r, normed_final, target_row):
    row_block = min(512, SEQ_LEN)

    def one_block(block_index):
        first_row = (block_index * row_block).astype(jnp.int32)
        rows_in = lax.dynamic_slice_in_dim(normed_final, first_row, row_block, 0)
        block_targets = lax.dynamic_slice_in_dim(target_row, first_row, row_block, 0)
        logits = low_back(jnp.einsum('rd,vd->rv', rows_in, table_r, precision=highest))
        spread = jax.nn.logsumexp(logits, axis=-1)
        picked = jnp.take_along_axis(logits, block_targets, axis=1)
        return jnp.sum(spread - picked[:, 0]) + second_weight * jnp.sum(spread - picked[:, 1])
    return jnp.sum(lax.map(jax.checkpoint(one_block), jnp.arange(SEQ_LEN // row_block, dtype=jnp.int32)))

def forward(table, blocks, gains, ids, targets, segments):
    table_r = low(table)
    layer_weights = [[low(matrix) for matrix in assemble(blocks[layer_index])] for layer_index in range(SECTIONS)]

    def one_sequence(running, inputs):
        seq_ids, seq_targets, seq_segments = inputs
        states = jnp.take(table_r, seq_ids, axis=0)
        for layer_index in range(SECTIONS):
            states = decoder_layer(states, layer_weights[layer_index], gains[2 * layer_index], gains[2 * layer_index + 1], seq_segments)
        normed_final = low(rms_scale(states, gains[2 * SECTIONS]))
        return (running + sequence_loss(table_r, normed_final, seq_targets), None)
    loss_sum, unused = lax.scan(one_sequence, jnp.zeros((), jnp.float32), (ids.reshape(-1, SEQ_LEN), targets.reshape(-1, SEQ_LEN, 2), segments.reshape(-1, SEQ_LEN)))
    return loss_sum / (MICRO * SEQS * SEQ_LEN)

def adam_step(weight, first, second, grad, decay):
    first_new = beta_first * first + (1.0 - beta_first) * grad
    second_new = beta_second * second + (1.0 - beta_second) * grad * grad
    weight_new = weight - adam_rate * (first_new / (jnp.sqrt(second_new) + adam_eps) + decay * weight)
    return (weight_new, first_new, second_new)

def reference(ids, targets, segments, table, table_m, table_v, blocks, left_stats, right_stats, left_root, right_root, gains, gains_m, gains_v):

    def objective(table_in, blocks_in, gains_in):
        return forward(table_in, blocks_in, gains_in, ids, targets, segments)
    loss, pull_back = jax.vjp(objective, table, blocks, gains)
    grad_table, grad_blocks, grad_gains = pull_back(jnp.ones((), jnp.float32))
    clip_norm = jnp.sqrt(jnp.sum(grad_table * grad_table) + jnp.sum(grad_blocks * grad_blocks) + jnp.sum(grad_gains * grad_gains))
    factor = clip_bound / jnp.maximum(clip_norm, clip_bound)
    grad_blocks = grad_blocks * factor
    left_new = stat_decay * left_stats + (1.0 - stat_decay) * jnp.einsum('sbij,sbkj->sbik', grad_blocks, grad_blocks, precision=highest)
    right_new = stat_decay * right_stats + (1.0 - stat_decay) * jnp.einsum('sbji,sbjk->sbik', grad_blocks, grad_blocks, precision=highest)
    direction = jnp.einsum('sbij,sbjk->sbik', left_root, jnp.einsum('sbij,sbjk->sbik', grad_blocks, right_root, precision=highest), precision=highest)
    blocks_new = blocks - shampoo_rate * direction
    table_new, table_m_new, table_v_new = adam_step(table, table_m, table_v, grad_table * factor, weight_decay)
    gains_new, gains_m_new, gains_v_new = adam_step(gains, gains_m, gains_v, grad_gains * factor, 0.0)
    return (loss, clip_norm, table_new, table_m_new, table_v_new, table_new.astype(jnp.bfloat16), blocks_new, blocks_new.astype(jnp.bfloat16), left_new, right_new, gains_new, gains_m_new, gains_v_new)
```

```python
import functools

import jax
import jax.numpy as jnp
from jax import lax
from jax.experimental import pallas as pl
from jax.experimental.pallas import tpu as pltpu
from jax.sharding import PartitionSpec as P

D = 768
HEADS = 12
HEAD_DIM = 64
FF = 2048
BS = 64
QUAD = 256

norm_eps = 1e-05
rope_base = 10000.0
clip_bound = 0.08
shampoo_rate = 0.1
adam_rate = 0.02
beta_first = 0.9
beta_second = 0.95
adam_eps = 1e-08
weight_decay = 0.1
stat_decay = 0.5
second_weight = 0.3
highest = lax.Precision.HIGHEST
MESH = pl.DeviceIdType.MESH
ORDER = ("blk", "shard", "section")
VMEM_MAX = 62 * 1024 * 1024
f32 = jnp.float32
bf16 = jnp.bfloat16


def remote(src,dst,ssem,rsem,dev):
    return pltpu.make_async_remote_copy(src_ref=src,dst_ref=dst,send_sem=ssem,recv_sem=rsem,device_id=dev,device_id_type=MESH)

def split_rows(R, step, frac):
    a=int(round(R*frac/step))*step
    return min(max(a,0),R)

def ag_kernel(B,H,parts,by_section,x_ref,o_ref,ssem,rsem,lsem):
    s=lax.axis_index("section"); b=lax.axis_index("blk"); h=lax.axis_index("shard")
    x1=h^1; y1=h^2; xy=h^3
    part=(1-s,b,h)
    xn=(s,b,x1); yn=(s,b,y1); lf=(s,b-1,h); rt=(s,b+1,h)
    has_l=b>0; has_r=b<B-1
    bar=pltpu.get_barrier_semaphore()
    for t in (part,xn,yn):
        pl.semaphore_signal(bar,inc=1,device_id=t,device_id_type=MESH)
    @pl.when(has_l)
    def _(): pl.semaphore_signal(bar,inc=1,device_id=lf,device_id_type=MESH)
    @pl.when(has_r)
    def _(): pl.semaphore_signal(bar,inc=1,device_id=rt,device_id_type=MESH)
    def slot(bb,hh,ss):
        return (ss*B+bb)*H+hh if by_section else (bb*H+hh)*2+ss
    def dst(p,bb,hh,ss): return o_ref.at[slot(bb,hh,ss),pl.ds(parts[p][0],parts[p][1])]
    def rs(p,bb,hh,ss): return rsem.at[p,slot(bb,hh,ss)]
    local=pltpu.make_async_copy(x_ref,o_ref.at[slot(b,h,s)],lsem.at[0])
    local.start()
    pl.semaphore_wait(bar,3+has_l.astype(jnp.int32)+has_r.astype(jnp.int32))
    pend=[]
    def send(p,bb,hh,ss,dev,cond=None,own=False,kind=0):
        i=len(pend)
        src=x_ref.at[pl.ds(parts[p][0],parts[p][1])] if own else dst(p,bb,hh,ss)
        cp=remote(src,dst(p,bb,hh,ss),ssem.at[i],rs(p,bb,hh,ss),dev)
        pend.append((cond,cp))
        if cond is None: cp.start()
        else:
            @pl.when(cond)
            def _(): cp.start()
    def wait(p,bb,hh,ss):
        remote(dst(p,bb,hh,ss),dst(p,bb,hh,ss),ssem.at[0],rs(p,bb,hh,ss),part).wait_recv()
    def andc(a,c):
        return c if a is None else jnp.logical_and(a,c)
    def on_arrive(cond,fn):
        if cond is None: fn()
        else: pl.when(cond)(fn)
    def group(cond,waits,sends):
        i0=len(pend)
        cps=[]
        for k,(p,bb,hh,dev,c,own) in enumerate(sends):
            src=x_ref.at[pl.ds(parts[p][0],parts[p][1])] if own else dst(p,bb,hh,s)
            cp=remote(src,dst(p,bb,hh,s),ssem.at[i0+k],rs(p,bb,hh,s),dev)
            cps.append((c,cp))
        def run():
            for (p,bb,hh) in waits: wait(p,bb,hh,s)
            for c,cp in cps:
                if c is None: cp.start()
                else: pl.when(c)(cp.start)
        on_arrive(cond,run)
        for c,cp in cps:
            cc=cond if c is None else (c if cond is None else jnp.logical_and(cond,c))
            pend.append((cc,cp))
    two=len(parts)>1
    group(None,[],[(0,b,h,rt,has_r,True),(0,b,h,lf,has_l,True),(0,b,h,xn,None,True),(0,b,h,yn,None,True)])
    if two:
        group(None,[],[(1,b,h,yn,None,True),(1,b,h,rt,has_r,True),(1,b,h,lf,has_l,True),(1,b,h,xn,None,True)])
    group(None,[],[(p,b,h,part,None,True) for p in range(len(parts))])
    if two:
        group(None,[(1,b,y1)],[(1,b,y1,rt,has_r,False),(1,b,y1,lf,has_l,False),(1,b,y1,xn,None,False),(1,b,y1,part,None,False)])
    group(None,[(0,b,x1)],[(0,b,x1,yn,None,False),(0,b,x1,part,None,False)])
    for d in range(1,B):
        cl=b>=d; cr=b+d<B
        group(cl,[(0,b-d,h)],[(0,b-d,h,rt,has_r,False),(0,b-d,h,xn,None,False),(0,b-d,h,yn,None,False),(0,b-d,h,part,None,False)])
        group(cr,[(0,b+d,h)],[(0,b+d,h,lf,has_l,False),(0,b+d,h,xn,None,False),(0,b+d,h,yn,None,False),(0,b+d,h,part,None,False)])
        if two:
            for hh in (h,y1):
                group(cl,[(1,b-d,hh)],[(1,b-d,hh,rt,has_r,False),(1,b-d,hh,xn,None,False),(1,b-d,hh,part,None,False)])
                group(cr,[(1,b+d,hh)],[(1,b+d,hh,lf,has_l,False),(1,b+d,hh,xn,None,False),(1,b+d,hh,part,None,False)])
        group(cl,[(0,b-d,x1)],[(0,b-d,x1,yn,None,False),(0,b-d,x1,part,None,False)])
        group(cr,[(0,b+d,x1)],[(0,b+d,x1,yn,None,False),(0,b+d,x1,part,None,False)])
    for d in range(B):
        for sg in ((1,-1) if d else (1,)):
            c=None if d==0 else (b+d<B if sg>0 else b>=d)
            bb=b+sg*d
            w=[(0,bb,y1),(0,bb,xy)]
            if two: w+= [(1,bb,x1),(1,bb,xy)]
            for e in w:
                group(c,[e],[(e[0],bb,e[2],part,None,False)])
    for bb in range(B):
        for hh in range(H):
            for p in range(len(parts)): wait(p,bb,hh,1-s)
    local.wait()
    for c,cp in pend:
        if c is None: cp.wait_send()
        else: pl.when(c)(cp.wait_send)

def all_gather32(x,B,H,cid,by_section=False,frac=0.636,vmem_out=False):
    R,C=x.shape
    step=16 if x.dtype==jnp.bfloat16 else 8
    a=split_rows(R,step,frac) if R>=4*step else R
    parts=[(0,a)]+([(a,R-a)] if a<R else [])
    n=2*B*H
    nsend=4+4+2+4+2+(B-1)*(8+4*4*1+4)+ (2*B-1)*4+16
    return pl.pallas_call(functools.partial(ag_kernel,B,H,parts,by_section),
        out_shape=jax.ShapeDtypeStruct((n,R,C),x.dtype),
        in_specs=[pl.BlockSpec(memory_space=pltpu.VMEM)],
        out_specs=pl.BlockSpec(memory_space=pl.ANY),
        scratch_shapes=[pltpu.SemaphoreType.DMA((nsend,)),pltpu.SemaphoreType.DMA((len(parts),n)),pltpu.SemaphoreType.DMA((1,))],
        compiler_params=pltpu.CompilerParams(collective_id=cid,has_side_effects=True),name=f"gather_{R}")(x)

def rs_kernel(B,H,parts,by_section,ranges,*refs):
    n_in=len(ranges)
    p_refs=refs[:n_in]; o_ref=refs[n_in]
    q,r1,ya,xa,za,xb,zb,yb,lsem,psem_s,psem_r,ssem,ya_s,xa_s,za_s,xb_s,zb_s,yb_s=refs[n_in+1:]
    s=lax.axis_index("section"); b=lax.axis_index("blk"); h=lax.axis_index("shard")
    x=h&1; y=h>>1
    part=(1-s,b,h); xn=(s,b,h^1); yn=(s,b,h^2); lf=(s,b-1,h); rt=(s,b+1,h)
    has_l=b>0; has_r=b<B-1
    bar=pltpu.get_barrier_semaphore()
    for t in (part,xn,yn):
        pl.semaphore_signal(bar,inc=1,device_id=t,device_id_type=MESH)
    @pl.when(has_l)
    def _(): pl.semaphore_signal(bar,inc=1,device_id=lf,device_id_type=MESH)
    @pl.when(has_r)
    def _(): pl.semaphore_signal(bar,inc=1,device_id=rt,device_id_type=MESH)
    (a0,an),(b0,bn)=parts
    def slot(bb,hh,ss):
        return (ss*B+bb)*H+hh if by_section else (bb*H+hh)*2+ss
    hs=[h^3,h^2,h^1,h]
    order=[(d,sg,k) for k in range(4) for d in range(B-1,-1,-1) for sg in ((1,-1) if d else (1,))]
    N=B*H
    def src(bb,hh,ss):
        return p_refs[0].at[slot(bb,hh,ss)]
    seq=[(bb,k) for k in range(4) for bb in range(B)]
    loads=[]
    for i,(bb,k) in enumerate(seq):
        hh=hs[k]
        cp=pltpu.make_async_copy(src(bb,hh,s),q.at[bb*H+hh],lsem.at[i]); cp.start()
        loads.append(cp)
    pl.semaphore_wait(bar,3+has_l.astype(jnp.int32)+has_r.astype(jnp.int32))
    psend=[]
    for i,(bb,k) in enumerate(seq):
        hh=hs[k]
        cp=remote(src(bb,hh,1-s),r1.at[bb*H+hh],psem_s.at[i],psem_r.at[i],part); cp.start()
        psend.append(cp)
    pend=[]; late=[]
    def flush():
        while late:
            c,cp=late.pop(0)
            if c is None: cp.start()
            else: pl.when(c)(cp.start)
    def queue(c,srcr,dstr,sem,dev):
        cp=remote(srcr,dstr,ssem.at[len(pend)],sem,dev)
        pend.append((c,cp)); late.append((c,cp))
    def add(dst,a,n):
        step=next(k for k in (128,112,96,80,64,48,32,16) if n%k==0)
        @pl.loop(0,n//step)
        def _(i):
            r=pl.ds(pl.multiple_of(i*step,step),step)
            dst[r,:]=dst[r,:]+a[r,:]
    A=pl.ds(a0,an); Bp=pl.ds(b0,bn)
    def got(dst,sem):
        remote(dst,dst,ssem.at[0],sem,part).wait_recv()
    R=an+bn
    for i,(bb,k) in enumerate(seq):
        hh=hs[k]
        loads[i].wait(); got(r1.at[bb*H+hh],psem_r.at[i])
        add(q.at[bb*H+hh],r1.at[bb*H+hh],R)
        flush()
        if k in (0,1):
            xx=(x^1) if k==0 else x
            queue(None,q.at[bb*H+hh,A],ya.at[bb*2+xx],ya_s.at[bb*2+xx],yn)
        if k in (0,2):
            yy=(y^1) if k==0 else y
            queue(None,q.at[bb*H+hh,Bp],xb.at[bb*2+yy],xb_s.at[bb*2+yy],xn)
    flush()
    for bb in range(B):
        for kk in range(2):
            xx=(x^1) if kk==0 else x
            hA=(h^1) if kk==0 else h
            yy=(y^1) if kk==0 else y
            hB=(h^2) if kk==0 else h
            if kk==0:
                got(ya.at[bb*2+xx],ya_s.at[bb*2+xx])
                add(q.at[bb*H+hA,A],ya.at[bb*2+xx],an)
                flush()
                queue(None,q.at[bb*H+hA,A],xa.at[bb],xa_s.at[bb],xn)
            got(xb.at[bb*2+yy],xb_s.at[bb*2+yy])
            add(q.at[bb*H+hB,Bp],xb.at[bb*2+yy],bn)
            flush()
    for bb in range(B):
        got(ya.at[bb*2+x],ya_s.at[bb*2+x])
        add(q.at[bb*H+h,A],ya.at[bb*2+x],an)
    def line_step(qref_of,zref_of,zsem_of,nn,d,sg,pre=None):
        t=b+sg*d
        c=(t<B) if sg>0 else (t>=0)
        hin=has_l if sg>0 else has_r
        dn=0 if sg>0 else 1
        dev=rt if sg>0 else lf
        def run():
            if pre is not None: pre(t)
            @pl.when(hin)
            def _():
                got(zref_of(dn,t),zsem_of(dn,t))
                add(qref_of(t),zref_of(dn,t),nn)
        pl.when(c)(run)
        flush()
        queue(c,qref_of(t),zref_of(dn,t),zsem_of(dn,t),dev)
    def final(qref_of,zref_of,zsem_of,nn):
        for dn,hin in ((0,has_l),(1,has_r)):
            @pl.when(hin)
            def _():
                got(zref_of(dn,b),zsem_of(dn,b))
                add(qref_of(b),zref_of(dn,b),nn)
    def pre_a(t):
        got(xa.at[t],xa_s.at[t])
        add(q.at[t*H+h,A],xa.at[t],an)
    fB=[]
    for yy,hh in ((y^1,h^2),(y,h)):
        fB.append((lambda t,hh=hh: q.at[t*H+hh,Bp], lambda dn,t,yy=yy: zb.at[(dn*B+t)*2+yy], lambda dn,t,yy=yy: zb_s.at[(dn*B+t)*2+yy], bn))
    fA=(lambda t: q.at[t*H+h,A], lambda dn,t: za.at[dn*B+t], lambda dn,t: za_s.at[dn*B+t], an)
    for d in range(B-1,0,-1):
        for sg in (1,-1):
            line_step(*fB[0],d,sg)
            line_step(*fB[1],d,sg)
            line_step(*fA,d,sg,pre_a)
    flush()
    pre_a(b)
    final(*fB[0])
    queue(None,q.at[b*H+(h^2),Bp],yb,yb_s.at[0],yn)
    final(*fA)
    flush()
    final(*fB[1])
    got(yb,yb_s.at[0])
    add(q.at[b*H+h,Bp],yb,bn)
    o_ref[...]=q[b*H+h]
    for cp in psend: cp.wait_send()
    for c,cp in pend:
        if c is None: cp.wait_send()
        else: pl.when(c)(cp.wait_send)

def reduce_scatter32(p,B,H,cid,by_section=False,frac=0.636):
    n,R,C=p.shape
    a=split_rows(R,16,frac)
    parts=((0,a),(a,R-a))
    V=lambda *s: pltpu.VMEM(s,p.dtype)
    D=lambda *s: pltpu.SemaphoreType.DMA(s)
    N=B*H
    an,bn=a,R-a
    nsend=8*B+B+6*(B-1)+8
    return pl.pallas_call(functools.partial(rs_kernel,B,H,parts,by_section,((0,n),)),
        out_shape=jax.ShapeDtypeStruct((R,C),p.dtype),
        in_specs=[pl.BlockSpec(memory_space=pl.ANY)],
        out_specs=pl.BlockSpec(memory_space=pltpu.VMEM),
        scratch_shapes=[V(N,R,C),V(N,R,C),V(2*B,an,C),V(B,an,C),V(2*B,an,C),V(2*B,bn,C),V(4*B,bn,C),V(bn,C),
           D(N),D(N),D(N),D(nsend),D(2*B),D(B),D(2*B),D(2*B),D(4*B),D(1)],
        compiler_params=pltpu.CompilerParams(collective_id=cid,has_side_effects=True,vmem_limit_bytes=63*1024*1024),name=f"scatter_{R}")(p)


def gather_all(value, cid, by_section=False):
    blk, shard = lax.axis_size("blk"), lax.axis_size("shard")
    if blk * shard <= 16 and shard == 4:
        return all_gather32(value, blk, shard, cid, by_section)
    names = ("section", "blk", "shard") if by_section else ORDER
    return lax.all_gather(value, names)


def scatter_all(value, cid, by_section=False):
    blk, shard = lax.axis_size("blk"), lax.axis_size("shard")
    if blk * shard <= 16 and shard == 4:
        return reduce_scatter32(value, blk, shard, cid, by_section)
    names = ("section", "blk", "shard") if by_section else ORDER
    return lax.psum_scatter(value, names, scatter_dimension=0)


def lookup_kernel(ids_ref, tab_ref, o_ref):
    rows = lax.broadcasted_iota(jnp.int32, (tab_ref.shape[0], ids_ref.shape[-1]), 0)
    hot = jnp.where(rows == ids_ref[0], 1.0, 0.0).astype(bf16)
    o_ref[0] = lax.dot_general(
        hot, tab_ref[...], (((0,), (0,)), ((), ())), preferred_element_type=f32
    ).astype(bf16)


def lookup(local_ids, table_low):
    count, tokens = local_ids.shape
    vocab = table_low.shape[0]
    return pl.pallas_call(
        lookup_kernel,
        grid=(count,),
        out_shape=jax.ShapeDtypeStruct((count, tokens, D), bf16),
        in_specs=[
            pl.BlockSpec((1, 1, tokens), lambda i: (i, 0, 0)),
            pl.BlockSpec((vocab, D), lambda i: (0, 0)),
        ],
        out_specs=pl.BlockSpec((1, tokens, D), lambda i: (i, 0, 0)),
        name="lookup",
    )(local_ids[:, None, :], table_low)


def spread_kernel(ids_ref, g_ref, base_ref, o_ref):
    rows = lax.broadcasted_iota(jnp.int32, (o_ref.shape[0], ids_ref.shape[-1]), 0)
    hot = jnp.where(rows == ids_ref[0], 1.0, 0.0).astype(bf16)

    @pl.when(pl.program_id(0) == 0)
    def _():
        o_ref[...] = base_ref[...]

    o_ref[...] += jnp.dot(hot, g_ref[0], preferred_element_type=f32)


def spread(local_ids, grads, base):
    count, tokens = local_ids.shape
    vocab = base.shape[0]
    return pl.pallas_call(
        spread_kernel,
        grid=(count,),
        out_shape=jax.ShapeDtypeStruct((vocab, D), f32),
        in_specs=[
            pl.BlockSpec((1, 1, tokens), lambda i: (i, 0, 0)),
            pl.BlockSpec((1, tokens, D), lambda i: (i, 0, 0)),
            pl.BlockSpec((vocab, D), lambda i: (0, 0)),
        ],
        out_specs=pl.BlockSpec((vocab, D), lambda i: (0, 0)),
        name="spread",
    )(local_ids[:, None, :], grads, base)


def stats_kernel(vocab, nf_ref, tab_ref, top_ref, sum_ref):
    logits = lax.dot_general(
        tab_ref[...], nf_ref[0], (((1,), (1,)), ((), ())), preferred_element_type=f32
    )
    rows = lax.broadcasted_iota(jnp.int32, logits.shape, 0)
    logits = jnp.where(rows < vocab, logits, -1e30)
    top = jnp.max(logits, axis=0, keepdims=True)
    top_ref[0] = top
    sum_ref[0] = jnp.sum(jnp.exp(logits - top), axis=0, keepdims=True)


def vocab_stats(normed, table_low, vocab):
    count, tokens, _ = normed.shape
    padded = table_low.shape[0]
    row = jax.ShapeDtypeStruct((count, 1, tokens), f32)
    return pl.pallas_call(
        functools.partial(stats_kernel, vocab),
        grid=(count,),
        out_shape=(row, row),
        in_specs=[
            pl.BlockSpec((1, tokens, D), lambda i: (i, 0, 0)),
            pl.BlockSpec((padded, D), lambda i: (0, 0)),
        ],
        out_specs=(
            pl.BlockSpec((1, 1, tokens), lambda i: (i, 0, 0)),
            pl.BlockSpec((1, 1, tokens), lambda i: (i, 0, 0)),
        ),
        name="vocab_stats",
    )(normed, table_low)


def vocab_kernel(vocab, scale, nf_ref, tab_ref, lse_ref, t0_ref, t1_ref, g_ref, acc_ref, pick_ref):
    logits = lax.dot_general(
        tab_ref[...], nf_ref[0], (((1,), (1,)), ((), ())), preferred_element_type=f32
    )
    rows = lax.broadcasted_iota(jnp.int32, logits.shape, 0)
    hits = jnp.where(rows == t0_ref[0], 1.0, 0.0) + jnp.where(rows == t1_ref[0], second_weight, 0.0)
    soft = jnp.exp(logits - lse_ref[0]) * (1.0 + second_weight)
    grad = jnp.where(rows < vocab, (soft - hits) * scale, 0.0).astype(bf16)

    @pl.when(pl.program_id(0) == 0)
    def _():
        acc_ref[...] = jnp.zeros_like(acc_ref)
        pick_ref[...] = jnp.zeros_like(pick_ref)

    pick_ref[...] += jnp.sum(hits * logits, axis=0, keepdims=True)
    g_ref[0] = lax.dot_general(
        grad, tab_ref[...], (((0,), (0,)), ((), ())), preferred_element_type=f32
    ).astype(bf16)
    acc_ref[...] += jnp.dot(grad, nf_ref[0], preferred_element_type=f32)


def vocab_grads(normed, table_low, log_total, first, second, vocab, scale):
    count, tokens, _ = normed.shape
    padded = table_low.shape[0]
    row = pl.BlockSpec((1, 1, tokens), lambda i: (i, 0, 0))
    return pl.pallas_call(
        functools.partial(vocab_kernel, vocab, scale),
        grid=(count,),
        out_shape=(
            jax.ShapeDtypeStruct((count, tokens, D), bf16),
            jax.ShapeDtypeStruct((padded, D), f32),
            jax.ShapeDtypeStruct((1, tokens), f32),
        ),
        in_specs=[
            pl.BlockSpec((1, tokens, D), lambda i: (i, 0, 0)),
            pl.BlockSpec((padded, D), lambda i: (0, 0)),
            row,
            row,
            row,
        ],
        out_specs=(
            pl.BlockSpec((1, tokens, D), lambda i: (i, 0, 0)),
            pl.BlockSpec((padded, D), lambda i: (0, 0)),
            pl.BlockSpec((1, tokens), lambda i: (0, 0)),
        ),
        name="vocab_grads",
    )(normed, table_low, log_total[:, None, :], first[:, None, :], second[:, None, :])


def place_of(index, shard):
    return (index % 2, index // (2 * shard), (index // 2) % shard)


def my_place():
    shard = lax.axis_size("shard")
    return (lax.axis_index("blk") * shard + lax.axis_index("shard")) * 2 + lax.axis_index("section")


def meet(reach, block, blocks, mine, shard, sign):
    barrier = pltpu.get_barrier_semaphore()
    above = [block + d < blocks for d in range(1, reach + 1)]
    below = [block >= d for d in range(1, reach + 1)]
    sources, targets = (below, above) if sign > 0 else (above, below)
    for d in range(1, reach + 1):

        @pl.when(sources[d - 1])
        def _():
            pl.semaphore_signal(
                barrier, inc=1, device_id=place_of(mine - sign * d, shard), device_id_type=MESH
            )

    @pl.when(targets[0])
    def _():
        pl.semaphore_wait(barrier, sum(held.astype(jnp.int32) for held in targets))


def half_masks(tokens):
    lane = lax.broadcasted_iota(jnp.int32, (tokens, 2 * HEAD_DIM), 1)
    return lane < HEAD_DIM


def allowed_mask(d, seg_ref, tokens):
    own = jnp.transpose(jnp.broadcast_to(seg_ref[0], (128, tokens)))[:, :1]
    allowed = own == seg_ref[d]
    if d == 0:
        row = lax.broadcasted_iota(jnp.int32, (tokens, tokens), 0)
        col = lax.broadcasted_iota(jnp.int32, (tokens, tokens), 1)
        allowed = allowed & (col <= row)
    return allowed


def attend_kernel(reach, blocks, q_ref, k_ref, v_ref, seg_ref, tot_ref, acc_ref, kr_ref, vr_ref,
                  send_sem, recv_sem):
    shard = lax.axis_size("shard")
    mine = (lax.axis_index("blk") * shard + lax.axis_index("shard")) * 2 + lax.axis_index("section")
    block = mine % blocks
    tokens = q_ref.shape[0]
    meet(reach, block, blocks, mine, shard, 1)

    def copies(d):
        target = place_of(mine + d, shard)
        return [
            pltpu.make_async_remote_copy(
                src_ref=source,
                dst_ref=target_ref.at[d - 1],
                send_sem=send_sem.at[d - 1, i],
                recv_sem=recv_sem.at[d - 1, i],
                device_id=target,
                device_id_type=MESH,
            )
            for i, (source, target_ref) in enumerate(((k_ref, kr_ref), (v_ref, vr_ref)))
        ]

    for d in range(reach, 0, -1):

        @pl.when(block + d < blocks)
        def _():
            for copy in copies(d):
                copy.start()

    scale = HEAD_DIM ** (-0.5)
    left = half_masks(tokens)
    zero = jnp.zeros((tokens, 2 * HEAD_DIM), bf16)

    def visit(d, keys, values):
        allowed = allowed_mask(d, seg_ref, tokens)

        @pl.loop(0, HEADS // 2)
        def _(pair):
            lanes = pl.ds(pl.multiple_of(pair * 128, 128), 128)
            q_pair, k_pair, v_pair = q_ref[:, lanes], keys[:, lanes], values[:, lanes]
            totals, sums = [], []
            for side in (left, ~left):
                scores = lax.dot_general(
                    jnp.where(side, q_pair, zero),
                    k_pair,
                    (((1,), (1,)), ((), ())),
                    preferred_element_type=f32,
                )
                expo = jnp.where(allowed, jnp.exp(scores * scale), 0.0)
                totals.append(jnp.sum(expo, axis=1, keepdims=True))
                sums.append(jnp.dot(expo.astype(bf16), v_pair, preferred_element_type=f32))
            total = jnp.where(left, totals[0], totals[1])
            added = jnp.where(left, sums[0], sums[1])
            if d == 0:
                tot_ref[:, lanes] = total
                acc_ref[:, lanes] = added
            else:
                tot_ref[:, lanes] += total
                acc_ref[:, lanes] += added

    visit(0, k_ref, v_ref)
    for d in range(1, reach + 1):

        @pl.when(block >= d)
        def _():
            for copy in copies(d):
                copy.wait_recv()
            visit(d, kr_ref.at[d - 1], vr_ref.at[d - 1])

    for d in range(1, reach + 1):

        @pl.when(block + d < blocks)
        def _():
            for copy in copies(d):
                copy.wait_send()


def attend(q, k, v, seg_rows, reach, blocks, cid):
    tokens = q.shape[0]
    wide = jax.ShapeDtypeStruct((tokens, D), f32)
    far = jax.ShapeDtypeStruct((reach, tokens, D), bf16)
    whole = pl.BlockSpec(memory_space=pltpu.VMEM)
    return pl.pallas_call(
        functools.partial(attend_kernel, reach, blocks),
        out_shape=(wide, wide, far, far),
        in_specs=[whole] * 4,
        out_specs=(whole,) * 4,
        scratch_shapes=[
            pltpu.SemaphoreType.DMA((reach, 2)),
            pltpu.SemaphoreType.DMA((reach, 2)),
        ],
        compiler_params=pltpu.CompilerParams(
            collective_id=cid, has_side_effects=True, vmem_limit_bytes=VMEM_MAX
        ),
        name="attend",
    )(q, k, v, seg_rows)


def attend_back_kernel(reach, blocks, q_ref, k_ref, v_ref, kr_ref, vr_ref, tot_ref, acc_ref, ga_ref,
                       seg_ref, dq_ref, dk_ref, dv_ref, gw, gt, far_k, far_v, got_k, got_v,
                       send_sem, recv_sem):
    shard = lax.axis_size("shard")
    mine = (lax.axis_index("blk") * shard + lax.axis_index("shard")) * 2 + lax.axis_index("section")
    block = mine % blocks
    tokens = q_ref.shape[0]
    meet(reach, block, blocks, mine, shard, -1)
    scale = HEAD_DIM ** (-0.5)
    left = half_masks(tokens)
    zero = jnp.zeros((tokens, 2 * HEAD_DIM), bf16)

    @pl.loop(0, HEADS // 2)
    def _(pair):
        lanes = pl.ds(pl.multiple_of(pair * 128, 128), 128)
        inverse = 1.0 / tot_ref[:, lanes]
        grad = ga_ref[:, lanes]
        gw[:, lanes] = (grad * inverse).astype(bf16)
        product = grad * acc_ref[:, lanes]
        first = jnp.sum(jnp.where(left, product, 0.0), axis=1, keepdims=True)
        second = jnp.sum(jnp.where(left, 0.0, product), axis=1, keepdims=True)
        gt[:, lanes] = -jnp.where(left, first, second) * inverse * inverse
        dq_ref[:, lanes] = jnp.zeros((tokens, 128), f32)

    def visit(d, keys, values, out_k, out_v):
        allowed = allowed_mask(d, seg_ref, tokens)

        @pl.loop(0, HEADS // 2)
        def _(pair):
            lanes = pl.ds(pl.multiple_of(pair * 128, 128), 128)
            q_pair, k_pair, v_pair, w_pair = q_ref[:, lanes], keys[:, lanes], values[:, lanes], gw[:, lanes]
            gt_pair = gt[:, lanes]
            dq, dk, dv = [], [], []
            for i, side in enumerate((left, ~left)):
                scores = lax.dot_general(
                    jnp.where(side, q_pair, zero),
                    k_pair,
                    (((1,), (1,)), ((), ())),
                    preferred_element_type=f32,
                )
                expo = jnp.where(allowed, jnp.exp(scores * scale), 0.0)
                probs = lax.dot_general(
                    jnp.where(side, w_pair, zero),
                    v_pair,
                    (((1,), (1,)), ((), ())),
                    preferred_element_type=f32,
                )
                part = (expo * (probs + gt_pair[:, i * HEAD_DIM : i * HEAD_DIM + 1])).astype(bf16)
                dq.append(jnp.dot(part, k_pair, preferred_element_type=f32))
                dk.append(
                    lax.dot_general(part, q_pair, (((0,), (0,)), ((), ())), preferred_element_type=f32)
                )
                dv.append(
                    lax.dot_general(
                        expo.astype(bf16), w_pair, (((0,), (0,)), ((), ())), preferred_element_type=f32
                    )
                )
            dq_ref[:, lanes] += jnp.where(left, dq[0], dq[1]) * scale
            out_k[:, lanes] = (jnp.where(left, dk[0], dk[1]) * scale).astype(out_k.dtype)
            out_v[:, lanes] = jnp.where(left, dv[0], dv[1]).astype(out_v.dtype)

    def copies(d):
        target = place_of(mine - d, shard)
        return [
            pltpu.make_async_remote_copy(
                src_ref=source.at[d - 1],
                dst_ref=target_ref.at[d - 1],
                send_sem=send_sem.at[d - 1, i],
                recv_sem=recv_sem.at[d - 1, i],
                device_id=target,
                device_id_type=MESH,
            )
            for i, (source, target_ref) in enumerate(((far_k, got_k), (far_v, got_v)))
        ]

    for d in range(reach, 0, -1):

        @pl.when(block >= d)
        def _():
            visit(d, kr_ref.at[d - 1], vr_ref.at[d - 1], far_k.at[d - 1], far_v.at[d - 1])
            for copy in copies(d):
                copy.start()

    visit(0, k_ref, v_ref, dk_ref, dv_ref)
    for d in range(reach, 0, -1):

        @pl.when(block + d < blocks)
        def _():
            for copy in copies(d):
                copy.wait_recv()
            dk_ref[...] += got_k[d - 1].astype(f32)
            dv_ref[...] += got_v[d - 1].astype(f32)

    for d in range(1, reach + 1):

        @pl.when(block >= d)
        def _():
            for copy in copies(d):
                copy.wait_send()


def attend_back(q, k, v, far_k, far_v, total, accum, grad, seg_rows, reach, blocks, cid):
    tokens = q.shape[0]
    wide = jax.ShapeDtypeStruct((tokens, D), f32)
    whole = pl.BlockSpec(memory_space=pltpu.VMEM)
    return pl.pallas_call(
        functools.partial(attend_back_kernel, reach, blocks),
        out_shape=(wide, wide, wide),
        in_specs=[whole] * 9,
        out_specs=(whole,) * 3,
        scratch_shapes=[pltpu.VMEM((tokens, D), bf16), pltpu.VMEM((tokens, D), f32)]
        + [pltpu.VMEM((reach, tokens, D), bf16)] * 4
        + [pltpu.SemaphoreType.DMA((reach, 2)), pltpu.SemaphoreType.DMA((reach, 2))],
        compiler_params=pltpu.CompilerParams(
            collective_id=cid, has_side_effects=True, vmem_limit_bytes=VMEM_MAX
        ),
        name="attend_back",
    )(q, k, v, far_k, far_v, total, accum, grad, seg_rows)


def matrix_layout():
    return ((D, 3 * D), (D, D), (D, 2 * FF), (FF, D))


def blocks_to_rows(blocks):
    count = blocks.shape[0]
    if count % 4:
        return blocks.reshape(-1, QUAD)
    quads = blocks.reshape(count // 4, 4, BS, BS).transpose(0, 2, 1, 3)
    return quads.reshape(-1, QUAD)


def rows_to_blocks(rows):
    count = rows.shape[0] * QUAD // (BS * BS)
    if count % 4:
        return rows.reshape(count, BS, BS)
    return rows.reshape(count // 4, BS, 4, BS).transpose(0, 2, 1, 3).reshape(count, BS, BS)


def rows_to_quads(rows, count):
    if count % 4:
        rows = rows.reshape(-1, 4, BS, BS).transpose(0, 2, 1, 3)
    return rows.reshape(-1, BS, QUAD)


def quads_to_rows(quads, count):
    if count % 4:
        quads = quads.reshape(-1, BS, 4, BS).transpose(0, 2, 1, 3)
    return quads.reshape(-1, count * BS * BS // QUAD, QUAD)


def quads_to_matrices(quads):
    matrices, offset = [], 0
    for rows, cols in matrix_layout():
        r, c = rows // BS, cols // QUAD
        part = quads[offset : offset + r * c].reshape(r, c, BS, QUAD)
        matrices.append(part.transpose(0, 2, 1, 3).reshape(rows, cols))
        offset += r * c
    return matrices


def matrices_to_quads(matrices):
    parts = []
    for matrix, (rows, cols) in zip(matrices, matrix_layout()):
        r, c = rows // BS, cols // QUAD
        parts.append(
            matrix.reshape(r, BS, c, QUAD).transpose(0, 2, 1, 3).reshape(r * c, BS, QUAD)
        )
    return jnp.concatenate(parts, axis=0)


def rms_scale(states, gain_row):
    return (
        states * lax.rsqrt(jnp.mean(states * states, axis=-1, keepdims=True) + norm_eps) * gain_row
    )


def rms_back(states, gain_row, grad_out):
    inverse = lax.rsqrt(jnp.mean(states * states, axis=-1, keepdims=True) + norm_eps)
    weighted = grad_out * gain_row
    grad_in = inverse * weighted - states * inverse * inverse * inverse * jnp.mean(
        weighted * states, axis=-1, keepdims=True
    )
    return (grad_in, jnp.sum(grad_out * states * inverse, axis=0))


def rope_tables(positions):
    half_dim = HEAD_DIM // 2
    frequency = rope_base ** (-jnp.arange(half_dim, dtype=f32) * 2.0 / HEAD_DIM)
    angles = positions.astype(f32)[:, None] * frequency[None, :]
    cosine, sine = jnp.cos(angles), jnp.sin(angles)
    return (
        jnp.concatenate([cosine, cosine], axis=-1)[:, None, :],
        jnp.concatenate([sine, sine], axis=-1)[:, None, :],
    )


def rotate(values, cosine, sine):
    half_dim = HEAD_DIM // 2
    turned = jnp.concatenate([-values[..., half_dim:], values[..., :half_dim]], axis=-1)
    return values * cosine + turned * sine


def rotate_back(grads, cosine, sine):
    half_dim = HEAD_DIM // 2
    scaled = grads * sine
    turned = jnp.concatenate([scaled[..., half_dim:], -scaled[..., :half_dim]], axis=-1)
    return grads * cosine + turned


def layer_forward(states, weights, gain_first, gain_second, tables, seg_rows, reach, blocks, cid):
    w_qkv, w_out, w_gate_up, w_down = weights
    rows = states.shape[0]
    normed = rms_scale(states, gain_first).astype(bf16)
    projected = jnp.dot(normed, w_qkv, preferred_element_type=f32)

    def turned(part):
        return rotate(part.reshape(rows, HEADS, HEAD_DIM), *tables).astype(bf16).reshape(rows, D)

    q = turned(projected[:, :D])
    k = turned(projected[:, D : 2 * D])
    v = projected[:, 2 * D :].astype(bf16)
    total, accum, far_k, far_v = attend(q, k, v, seg_rows, reach, blocks, cid)
    attended = (accum / total).astype(bf16)
    mixed = states + jnp.dot(attended, w_out, preferred_element_type=f32)
    normed_mid = rms_scale(mixed, gain_second).astype(bf16)
    gate_up = jnp.dot(normed_mid, w_gate_up, preferred_element_type=f32)
    gate, upper = gate_up[:, :FF], gate_up[:, FF:]
    hidden = (jax.nn.silu(gate) * upper).astype(bf16)
    output = mixed + jnp.dot(hidden, w_down, preferred_element_type=f32)
    return output, (
        states, normed, q, k, v, far_k, far_v, total, accum, attended, mixed, normed_mid, gate,
        upper, hidden,
    )


def layer_backward(cache, grad_out, weights, gain_first, gain_second, tables, seg_rows, reach, blocks, cid):
    (
        states, normed, q, k, v, far_k, far_v, total, accum, attended, mixed, normed_mid, gate,
        upper, hidden,
    ) = cache
    w_qkv, w_out, w_gate_up, w_down = weights
    rows = states.shape[0]

    def outer(left_side, right_side):
        return jnp.einsum(
            "rd,rf->df", left_side, right_side, preferred_element_type=f32
        ).astype(bf16)

    def through(grad, weight):
        return jnp.einsum("rf,df->rd", grad, weight, preferred_element_type=f32)

    grad_low = grad_out.astype(bf16)
    grad_w_down = outer(hidden, grad_low)
    grad_hidden = through(grad_low, w_down)
    sig = jax.nn.sigmoid(gate)
    grad_gate = grad_hidden * upper * sig * (1.0 + gate * (1.0 - sig))
    grad_up = grad_hidden * gate * sig
    grad_gate_up = jnp.concatenate([grad_gate, grad_up], axis=-1).astype(bf16)
    grad_w_gate_up = outer(normed_mid, grad_gate_up)
    grad_mid_norm, grad_gain_second = rms_back(mixed, gain_second, through(grad_gate_up, w_gate_up))
    grad_mixed = grad_out + grad_mid_norm
    grad_att = grad_mixed.astype(bf16)
    grad_w_out = outer(attended, grad_att)
    grad_attended = through(grad_att, w_out)
    grad_q, grad_k, grad_v = attend_back(
        q, k, v, far_k, far_v, total, accum, grad_attended, seg_rows, reach, blocks, cid
    )

    def unturned(part):
        return rotate_back(part.reshape(rows, HEADS, HEAD_DIM), *tables).reshape(rows, D)

    grad_qkv = jnp.concatenate([unturned(grad_q), unturned(grad_k), grad_v], axis=-1).astype(bf16)
    grad_w_qkv = outer(normed, grad_qkv)
    grad_in_norm, grad_gain_first = rms_back(states, gain_first, through(grad_qkv, w_qkv))
    return (
        grad_mixed + grad_in_norm,
        (grad_w_qkv, grad_w_out, grad_w_gate_up, grad_w_down),
        grad_gain_first,
        grad_gain_second,
    )


def adam_step(weight, first, second, grad_in, decay):
    first_new = beta_first * first + (1.0 - beta_first) * grad_in
    second_new = beta_second * second + (1.0 - beta_second) * grad_in * grad_in
    weight_new = weight - adam_rate * (
        first_new / (jnp.sqrt(second_new) + adam_eps) + decay * weight
    )
    return (weight_new, first_new, second_new)


def on_device(ids, targets, segments, table, table_m, table_v, blocks, left_stats, right_stats,
              left_root, right_root, gains, gains_m, gains_v):
    blk, shard = lax.axis_size("blk"), lax.axis_size("shard")
    section = lax.axis_index("section")
    blk_index, shard_index = lax.axis_index("blk"), lax.axis_index("shard")
    devices = 2 * blk * shard
    micro, _, tok_rows = ids.shape
    seq_len = segments.shape[2]
    all_tokens = micro * shard * seq_len
    tokens = all_tokens // devices
    seq_blocks = seq_len // tokens
    reach = pl.cdiv(seq_len // 2 - 1, tokens)
    vocab = table.shape[0]
    padded = pl.cdiv(vocab, 128) * 128
    own_blocks = blocks.shape[1]

    mine = my_place()
    seg_own = lax.dynamic_slice_in_dim(segments[:, 0, :], blk_index * tok_rows, tok_rows, axis=1)
    packed = jnp.stack(
        [ids[:, 0, :], targets[:, 0, :, 0], targets[:, 0, :, 1], seg_own], axis=0
    ).reshape(4 * micro, tok_rows)
    shared = lax.all_gather(packed, ("blk", "shard")).reshape(blk, shard, 4, micro, tok_rows)
    shared = shared.transpose(2, 3, 1, 0, 4).reshape(4, devices, tokens)
    first_row = ((section * blk + blk_index) * shard + shard_index) * vocab
    local_ids, local_first, local_second = (shared[i] - first_row for i in range(3))

    def mark(values):
        return jnp.where((values >= 0) & (values < vocab), values, -1)

    local_ids, local_first, local_second = mark(local_ids), mark(local_first), mark(local_second)
    seg_index = jnp.maximum(mine - jnp.arange(reach + 1), 0)
    seg_rows = jnp.take(shared[3], seg_index, axis=0).astype(f32)[:, None, :]

    rows_low = blocks_to_rows(blocks[0].astype(bf16))
    gathered = gather_all(rows_low, 0, by_section=True)
    gathered = gathered.reshape(2, blk * shard * rows_low.shape[0], QUAD)
    table_low = jnp.pad(table.astype(bf16), ((0, padded - vocab), (0, 0)))
    looked = lookup(local_ids, table_low)
    states = scatter_all(looked, 1).astype(f32)

    weights = [quads_to_matrices(rows_to_quads(gathered[l], own_blocks)) for l in range(2)]
    positions = (mine % seq_blocks) * tokens + jnp.arange(tokens, dtype=jnp.int32)
    tables = rope_tables(positions)
    caches = []
    for l in range(2):
        states, cache = layer_forward(
            states, weights[l], gains[2 * l], gains[2 * l + 1], tables, seg_rows, reach, seq_blocks, 2
        )
        caches.append(cache)
    final_gain = gains[gains.shape[0] - 1]
    normed_own = rms_scale(states, final_gain).astype(bf16)
    normed = gather_all(normed_own, 3)
    top, spread_sum = vocab_stats(normed, table_low, vocab)
    stats = gather_all(jnp.concatenate([top[:, 0], spread_sum[:, 0]], axis=0), 4)
    tops, sums = stats[:, :devices], stats[:, devices:]
    largest = jnp.max(tops, axis=0)
    log_total = largest + jnp.log(jnp.sum(sums * jnp.exp(tops - largest), axis=0))
    inv_count = 1.0 / all_tokens
    grad_rows, head_term, picks = vocab_grads(
        normed, table_low, log_total, local_first, local_second, vocab, inv_count
    )
    own_log = lax.dynamic_index_in_dim(log_total, mine, 0, keepdims=False)
    loss_part = (1.0 + second_weight) * jnp.sum(own_log) - jnp.sum(picks)
    grad_final = scatter_all(grad_rows, 1).astype(f32)
    grad_states, grad_gain_final = rms_back(states, final_gain, grad_final)
    gain_grads = [None] * 5
    gain_grads[4] = grad_gain_final
    quads = [None, None]
    for l in (1, 0):
        grad_states, grads, gain_grads[2 * l], gain_grads[2 * l + 1] = layer_backward(
            caches[l], grad_states, weights[l], gains[2 * l], gains[2 * l + 1], tables, seg_rows,
            reach, seq_blocks, 5
        )
        quads[l] = quads_to_rows(matrices_to_quads(grads), own_blocks)
    block_rows = scatter_all(jnp.concatenate(quads, axis=0), 6, by_section=True).astype(f32)
    grad_embed = gather_all(grad_states.astype(bf16), 3)
    table_own = spread(local_ids, grad_embed, head_term)[:vocab]
    block_own = rows_to_blocks(block_rows)
    square_sum = jnp.sum(table_own * table_own) + jnp.sum(block_rows * block_rows)
    small = jnp.stack(
        gain_grads
        + [jnp.full((D,), square_sum), jnp.full((D,), loss_part), jnp.zeros((D,), f32)]
    )
    summed = jnp.sum(gather_all(small, 7), axis=0)
    gain_grad = summed[:5]
    clip_norm = jnp.sqrt(summed[5, 0] + jnp.sum(gain_grad * gain_grad))
    factor = clip_bound / jnp.maximum(clip_norm, clip_bound)
    loss = summed[6, 0] * inv_count
    grad_blocks = block_own * factor
    left_new = stat_decay * left_stats[0] + (1.0 - stat_decay) * jnp.einsum(
        "bij,bkj->bik", grad_blocks, grad_blocks, precision=highest
    )
    right_new = stat_decay * right_stats[0] + (1.0 - stat_decay) * jnp.einsum(
        "bji,bjk->bik", grad_blocks, grad_blocks, precision=highest
    )
    direction = jnp.einsum(
        "bij,bjk->bik",
        left_root[0],
        jnp.einsum("bij,bjk->bik", grad_blocks, right_root[0], precision=highest),
        precision=highest,
    )
    blocks_new = blocks[0] - shampoo_rate * direction
    table_new, table_m_new, table_v_new = adam_step(
        table, table_m, table_v, table_own * factor, weight_decay
    )
    gains_new, gains_m_new, gains_v_new = adam_step(
        gains, gains_m, gains_v, gain_grad * factor, 0.0
    )
    return (
        loss, clip_norm, table_new, table_m_new, table_v_new, table_new.astype(bf16),
        blocks_new[None], blocks_new[None].astype(bf16), left_new[None], right_new[None],
        gains_new, gains_m_new, gains_v_new,
    )


def solution(mesh):
    rows = P(("section", "blk", "shard"), None)
    square = P("section", ("blk", "shard"), None, None)
    return jax.shard_map(
        on_device,
        mesh=mesh,
        in_specs=(
            P(None, "shard", "blk"),
            P(None, "shard", "blk", None),
            P(None, "shard", None),
            rows, rows, rows,
            square, square, square, square, square,
            P(), P(), P(),
        ),
        out_specs=(
            P(), P(),
            rows, rows, rows, rows,
            square, square, square, square,
            P(), P(), P(),
        ),
        check_vma=False,
    )
```

```python
import functools

import jax
import jax.numpy as jnp
from jax import lax
from jax.experimental import pallas as pl
from jax.experimental.pallas import tpu as pltpu
from jax.sharding import PartitionSpec as P

D = 768
HEADS = 12
HEAD_DIM = 64
FF = 2048
BS = 64
QUAD = 256

norm_eps = 1e-05
rope_base = 10000.0
clip_bound = 0.08
shampoo_rate = 0.1
adam_rate = 0.02
beta_first = 0.9
beta_second = 0.95
adam_eps = 1e-08
weight_decay = 0.1
stat_decay = 0.5
second_weight = 0.3
highest = lax.Precision.HIGHEST
MESH = pl.DeviceIdType.MESH
ORDER = ("blk", "shard", "section")
VMEM_MAX = 62 * 1024 * 1024
f32 = jnp.float32
bf16 = jnp.bfloat16


def remote(src,dst,ssem,rsem,dev):
    return pltpu.make_async_remote_copy(src_ref=src,dst_ref=dst,send_sem=ssem,recv_sem=rsem,device_id=dev,device_id_type=MESH)

def split_rows(R, step, frac):
    a=int(round(R*frac/step))*step
    return min(max(a,0),R)

def ag_kernel(B,H,parts,by_section,x_ref,o_ref,ssem,rsem,lsem):
    s=lax.axis_index("section"); b=lax.axis_index("blk"); h=lax.axis_index("shard")
    x1=h^1; y1=h^2; xy=h^3
    part=(1-s,b,h)
    xn=(s,b,x1); yn=(s,b,y1); lf=(s,b-1,h); rt=(s,b+1,h)
    has_l=b>0; has_r=b<B-1
    bar=pltpu.get_barrier_semaphore()
    for t in (part,xn,yn):
        pl.semaphore_signal(bar,inc=1,device_id=t,device_id_type=MESH)
    @pl.when(has_l)
    def _(): pl.semaphore_signal(bar,inc=1,device_id=lf,device_id_type=MESH)
    @pl.when(has_r)
    def _(): pl.semaphore_signal(bar,inc=1,device_id=rt,device_id_type=MESH)
    def slot(bb,hh,ss):
        return (ss*B+bb)*H+hh if by_section else (bb*H+hh)*2+ss
    def dst(p,bb,hh,ss): return o_ref.at[slot(bb,hh,ss),pl.ds(parts[p][0],parts[p][1])]
    def rs(p,bb,hh,ss): return rsem.at[p,slot(bb,hh,ss)]
    local=pltpu.make_async_copy(x_ref,o_ref.at[slot(b,h,s)],lsem.at[0])
    local.start()
    pl.semaphore_wait(bar,3+has_l.astype(jnp.int32)+has_r.astype(jnp.int32))
    pend=[]
    def send(p,bb,hh,ss,dev,cond=None,own=False,kind=0):
        i=len(pend)
        src=x_ref.at[pl.ds(parts[p][0],parts[p][1])] if own else dst(p,bb,hh,ss)
        cp=remote(src,dst(p,bb,hh,ss),ssem.at[i],rs(p,bb,hh,ss),dev)
        pend.append((cond,cp))
        if cond is None: cp.start()
        else:
            @pl.when(cond)
            def _(): cp.start()
    def wait(p,bb,hh,ss):
        remote(dst(p,bb,hh,ss),dst(p,bb,hh,ss),ssem.at[0],rs(p,bb,hh,ss),part).wait_recv()
    def andc(a,c):
        return c if a is None else jnp.logical_and(a,c)
    def on_arrive(cond,fn):
        if cond is None: fn()
        else: pl.when(cond)(fn)
    def group(cond,waits,sends):
        i0=len(pend)
        cps=[]
        for k,(p,bb,hh,dev,c,own) in enumerate(sends):
            src=x_ref.at[pl.ds(parts[p][0],parts[p][1])] if own else dst(p,bb,hh,s)
            cp=remote(src,dst(p,bb,hh,s),ssem.at[i0+k],rs(p,bb,hh,s),dev)
            cps.append((c,cp))
        def run():
            for (p,bb,hh) in waits: wait(p,bb,hh,s)
            for c,cp in cps:
                if c is None: cp.start()
                else: pl.when(c)(cp.start)
        on_arrive(cond,run)
        for c,cp in cps:
            cc=cond if c is None else (c if cond is None else jnp.logical_and(cond,c))
            pend.append((cc,cp))
    two=len(parts)>1
    group(None,[],[(0,b,h,rt,has_r,True),(0,b,h,lf,has_l,True),(0,b,h,xn,None,True),(0,b,h,yn,None,True)])
    if two:
        group(None,[],[(1,b,h,yn,None,True),(1,b,h,rt,has_r,True),(1,b,h,lf,has_l,True),(1,b,h,xn,None,True)])
    group(None,[],[(p,b,h,part,None,True) for p in range(len(parts))])
    if two:
        group(None,[(1,b,y1)],[(1,b,y1,rt,has_r,False),(1,b,y1,lf,has_l,False),(1,b,y1,xn,None,False),(1,b,y1,part,None,False)])
    group(None,[(0,b,x1)],[(0,b,x1,yn,None,False),(0,b,x1,part,None,False)])
    for d in range(1,B):
        cl=b>=d; cr=b+d<B
        group(cl,[(0,b-d,h)],[(0,b-d,h,rt,has_r,False),(0,b-d,h,xn,None,False),(0,b-d,h,yn,None,False),(0,b-d,h,part,None,False)])
        group(cr,[(0,b+d,h)],[(0,b+d,h,lf,has_l,False),(0,b+d,h,xn,None,False),(0,b+d,h,yn,None,False),(0,b+d,h,part,None,False)])
        if two:
            for hh in (h,y1):
                group(cl,[(1,b-d,hh)],[(1,b-d,hh,rt,has_r,False),(1,b-d,hh,xn,None,False),(1,b-d,hh,part,None,False)])
                group(cr,[(1,b+d,hh)],[(1,b+d,hh,lf,has_l,False),(1,b+d,hh,xn,None,False),(1,b+d,hh,part,None,False)])
        group(cl,[(0,b-d,x1)],[(0,b-d,x1,yn,None,False),(0,b-d,x1,part,None,False)])
        group(cr,[(0,b+d,x1)],[(0,b+d,x1,yn,None,False),(0,b+d,x1,part,None,False)])
    for d in range(B):
        for sg in ((1,-1) if d else (1,)):
            c=None if d==0 else (b+d<B if sg>0 else b>=d)
            bb=b+sg*d
            w=[(0,bb,y1),(0,bb,xy)]
            if two: w+= [(1,bb,x1),(1,bb,xy)]
            for e in w:
                group(c,[e],[(e[0],bb,e[2],part,None,False)])
    for bb in range(B):
        for hh in range(H):
            for p in range(len(parts)): wait(p,bb,hh,1-s)
    local.wait()
    for c,cp in pend:
        if c is None: cp.wait_send()
        else: pl.when(c)(cp.wait_send)

def all_gather32(x,B,H,cid,by_section=False,frac=0.636,vmem_out=False):
    R,C=x.shape
    step=16 if x.dtype==jnp.bfloat16 else 8
    a=split_rows(R,step,frac) if R>=4*step else R
    parts=[(0,a)]+([(a,R-a)] if a<R else [])
    n=2*B*H
    nsend=4+4+2+4+2+(B-1)*(8+4*4*1+4)+ (2*B-1)*4+16
    return pl.pallas_call(functools.partial(ag_kernel,B,H,parts,by_section),
        out_shape=jax.ShapeDtypeStruct((n,R,C),x.dtype),
        in_specs=[pl.BlockSpec(memory_space=pltpu.VMEM)],
        out_specs=pl.BlockSpec(memory_space=pl.ANY),
        scratch_shapes=[pltpu.SemaphoreType.DMA((nsend,)),pltpu.SemaphoreType.DMA((len(parts),n)),pltpu.SemaphoreType.DMA((1,))],
        compiler_params=pltpu.CompilerParams(collective_id=cid,has_side_effects=True),name=f"gather_{R}")(x)

def rs_kernel(B,H,parts,by_section,p_ref,o_ref,*refs):
    q,r1,ya,xa,za,xb,zb,yb,lsem,psem_s,psem_r,ssem,ya_s,xa_s,za_s,xb_s,zb_s,yb_s=refs
    s=lax.axis_index("section"); b=lax.axis_index("blk"); h=lax.axis_index("shard")
    x=h&1; y=h>>1
    part=(1-s,b,h); xn=(s,b,h^1); yn=(s,b,h^2); lf=(s,b-1,h); rt=(s,b+1,h)
    has_l=b>0; has_r=b<B-1
    bar=pltpu.get_barrier_semaphore()
    for t in (part,xn,yn):
        pl.semaphore_signal(bar,inc=1,device_id=t,device_id_type=MESH)
    @pl.when(has_l)
    def _(): pl.semaphore_signal(bar,inc=1,device_id=lf,device_id_type=MESH)
    @pl.when(has_r)
    def _(): pl.semaphore_signal(bar,inc=1,device_id=rt,device_id_type=MESH)
    (a0,an),(b0,bn)=parts
    R=an+bn
    A=pl.ds(a0,an); Bp=pl.ds(b0,bn)
    def slot(bb,hh,ss):
        return (ss*B+bb)*H+hh if by_section else (bb*H+hh)*2+ss
    low=b<B//2
    order=[]
    for i in range(B-1):
        down=B-1-i
        order.append(jnp.where(low,down-(down<=b).astype(jnp.int32),i+(i>=b).astype(jnp.int32)))
    order.append(b)
    hs=[h^3,h^2,h^1,h]
    loads={}
    for i,t in enumerate(order):
        for k in range(4):
            cp=pltpu.make_async_copy(p_ref.at[slot(t,hs[k],s)],q.at[t*H+hs[k]],lsem.at[i*4+k]); cp.start()
            loads[i,k]=cp
    pl.semaphore_wait(bar,3+has_l.astype(jnp.int32)+has_r.astype(jnp.int32))
    psend={}
    for i,t in enumerate(order):
        for k in range(4):
            cp=remote(p_ref.at[slot(t,hs[k],1-s)],r1.at[t*H+hs[k]],psem_s.at[i*4+k],psem_r.at[i*4+k],part); cp.start()
            psend[i,k]=cp
    pend=[]; late=[]
    def flush():
        while late:
            c,cp=late.pop(0)
            if c is None: cp.start()
            else: pl.when(c)(cp.start)
    def queue(c,srcr,dstr,sem,dev):
        cp=remote(srcr,dstr,ssem.at[len(pend)],sem,dev)
        pend.append((c,cp)); late.append((c,cp))
    def add(dst,a,n):
        step=next(k for k in (128,112,96,80,64,48,32,16) if n%k==0)
        @pl.loop(0,n//step)
        def _(i):
            r=pl.ds(pl.multiple_of(i*step,step),step)
            dst[r,:]=dst[r,:]+a[r,:]
    def got(dst,sem):
        remote(dst,dst,ssem.at[0],sem,part).wait_recv()
    def first(i):
        t=order[i]
        for k in range(4):
            hh=hs[k]
            loads[i,k].wait(); psend[i,k].wait_recv()
            add(q.at[t*H+hh],r1.at[t*H+hh],R)
            flush()
            if k in (0,1):
                xx=(x^1) if k==0 else x
                queue(None,q.at[t*H+hh,A],ya.at[t*2+xx],ya_s.at[t*2+xx],yn)
            if k in (0,2):
                yy=(y^1) if k==0 else y
                queue(None,q.at[t*H+hh,Bp],xb.at[t*2+yy],xb_s.at[t*2+yy],xn)
    def second(i):
        t=order[i]
        xx=x^1
        got(ya.at[t*2+xx],ya_s.at[t*2+xx])
        add(q.at[t*H+hs[2],A],ya.at[t*2+xx],an)
        flush()
        queue(None,q.at[t*H+hs[2],A],xa.at[t],xa_s.at[t],xn)
        got(xb.at[t*2+(y^1)],xb_s.at[t*2+(y^1)])
        add(q.at[t*H+hs[1],Bp],xb.at[t*2+(y^1)],bn)
        flush()
        got(ya.at[t*2+x],ya_s.at[t*2+x])
        add(q.at[t*H+h,A],ya.at[t*2+x],an)
        got(xb.at[t*2+y],xb_s.at[t*2+y])
        add(q.at[t*H+h,Bp],xb.at[t*2+y],bn)
    lines=[(hs[1],Bp,bn,lambda d,t: zb.at[(d*B+t)*2+(y^1)],lambda d,t: zb_s.at[(d*B+t)*2+(y^1)]),
           (h,Bp,bn,lambda d,t: zb.at[(d*B+t)*2+y],lambda d,t: zb_s.at[(d*B+t)*2+y]),
           (h,A,an,lambda d,t: za.at[d*B+t],lambda d,t: za_s.at[d*B+t])]
    def third(i):
        t=order[i]
        for j,(hh,rows,n,zr,zs) in enumerate(lines):
            if j==2:
                got(xa.at[t],xa_s.at[t])
                add(q.at[t*H+h,A],xa.at[t],an)
            for d,c,hin,dev in ((0,t>b,has_l,rt),(1,t<b,has_r,lf)):
                @pl.when(jnp.logical_and(c,hin))
                def _():
                    got(zr(d,t),zs(d,t))
                    add(q.at[t*H+hh,rows],zr(d,t),n)
            flush()
            for d,c,hin,dev in ((0,t>b,has_l,rt),(1,t<b,has_r,lf)):
                queue(c,q.at[t*H+hh,rows],zr(d,t),zs(d,t),dev)
    def last(j):
        hh,rows,n,zr,zs=lines[j]
        for d,hin in ((0,has_l),(1,has_r)):
            @pl.when(hin)
            def _():
                got(zr(d,b),zs(d,b))
                add(q.at[b*H+hh,rows],zr(d,b),n)
    for i in range(B+2):
        if i<B: first(i)
        if 1<=i<B+1: second(i-1)
        if 2<=i<B+1: third(i-2)
    flush()
    last(0)
    queue(None,q.at[b*H+hs[1],Bp],yb,yb_s.at[0],yn)
    got(xa.at[b],xa_s.at[b])
    add(q.at[b*H+h,A],xa.at[b],an)
    flush()
    last(1)
    last(2)
    got(yb,yb_s.at[0])
    add(q.at[b*H+h,Bp],yb,bn)
    o_ref[...]=q[b*H+h]
    for cp in psend.values(): cp.wait_send()
    for c,cp in pend:
        if c is None: cp.wait_send()
        else: pl.when(c)(cp.wait_send)

def reduce_scatter32(p,B,H,cid,by_section=False,frac=0.636):
    n,R,C=p.shape
    a=split_rows(R,16,frac)
    parts=((0,a),(a,R-a))
    V=lambda *s: pltpu.VMEM(s,p.dtype)
    D=lambda *s: pltpu.SemaphoreType.DMA(s)
    N=B*H
    an,bn=a,R-a
    nsend=4*B+B+6*(B-1)+2
    return pl.pallas_call(functools.partial(rs_kernel,B,H,parts,by_section),
        out_shape=jax.ShapeDtypeStruct((R,C),p.dtype),
        in_specs=[pl.BlockSpec(memory_space=pl.ANY)],
        out_specs=pl.BlockSpec(memory_space=pltpu.VMEM),
        scratch_shapes=[V(N,R,C),V(N,R,C),V(2*B,an,C),V(B,an,C),V(2*B,an,C),V(2*B,bn,C),V(4*B,bn,C),V(bn,C),
           D(N),D(N),D(N),D(nsend),D(2*B),D(B),D(2*B),D(2*B),D(4*B),D(1)],
        compiler_params=pltpu.CompilerParams(collective_id=cid,has_side_effects=True,vmem_limit_bytes=63*1024*1024),name=f"scatter_{R}")(p)

def swap_kernel(n,join,x_ref,o_ref,got,total,ssem,rsem,ssem2,rsem2):
    B,H=lax.axis_size("blk"),lax.axis_size("shard")
    me=(lax.axis_index("blk")*H+lax.axis_index("shard"))*2+lax.axis_index("section")
    bar=pltpu.get_barrier_semaphore()
    def place(k):
        t=(me+k)%n
        return t,(t%2,t//(2*H),(t//2)%H)
    @pl.loop(1,n)
    def _(k):
        pl.semaphore_signal(bar,inc=1,device_id=place(k)[1],device_id_type=MESH)
    pl.semaphore_wait(bar,n-1)
    if join is None:
        def copy(k):
            return remote(x_ref,o_ref.at[me],ssem.at[k],rsem.at[k],place(k)[1])
        @pl.loop(1,n)
        def _(k): copy(k).start()
        o_ref[me]=x_ref[...]
        @pl.loop(1,n)
        def _(k): copy(k).wait()
        return
    def piece(k):
        t,dev=place(k)
        return remote(x_ref.at[t],got.at[me],ssem.at[k],rsem.at[k],dev)
    def spread(k):
        return remote(total,o_ref.at[me],ssem2.at[k],rsem2.at[k],place(k)[1])
    @pl.loop(1,n)
    def _(k): piece(k).start()
    got[me]=x_ref[me]
    @pl.loop(1,n)
    def _(k): piece(k).wait()
    total[...]=join(got)
    o_ref[me]=total[...]
    @pl.loop(1,n)
    def _(k): spread(k).start()
    @pl.loop(1,n)
    def _(k): spread(k).wait()

def swap_all(x,n,cid,join=None,out_rows=None,name="swap"):
    whole=pl.BlockSpec(memory_space=pltpu.VMEM)
    D=pltpu.SemaphoreType.DMA
    C=x.shape[-1]
    R=x.shape[-2]
    out=(n,R,C) if join is None else (n,out_rows,C)
    small=(8,128) if join is None else (out_rows,C)
    return pl.pallas_call(functools.partial(swap_kernel,n,join),
        out_shape=jax.ShapeDtypeStruct(out,x.dtype),in_specs=[whole],out_specs=whole,
        scratch_shapes=[pltpu.VMEM((8,128) if join is None else (n,R,C),x.dtype),pltpu.VMEM(small,x.dtype),D((n,)),D((n,)),D((n,)),D((n,))],
        compiler_params=pltpu.CompilerParams(collective_id=cid,has_side_effects=True),name=name)(x)


def join_stats(got):
    tops=got[:,0:1,:]
    largest=jnp.max(tops,axis=0)
    return largest+jnp.log(jnp.sum(got[:,1:2,:]*jnp.exp(tops-largest),axis=0))


def join_sum(got):
    return jnp.sum(got[...],axis=0)


def gather_all(value, cid, by_section=False):
    blk, shard = lax.axis_size("blk"), lax.axis_size("shard")
    if blk * shard <= 16 and shard == 4:
        return all_gather32(value, blk, shard, cid, by_section)
    names = ("section", "blk", "shard") if by_section else ORDER
    return lax.all_gather(value, names)


def scatter_all(value, cid, by_section=False):
    blk, shard = lax.axis_size("blk"), lax.axis_size("shard")
    if blk * shard <= 16 and shard == 4:
        return reduce_scatter32(value, blk, shard, cid, by_section)
    names = ("section", "blk", "shard") if by_section else ORDER
    return lax.psum_scatter(value, names, scatter_dimension=0)


def lookup_kernel(ids_ref, tab_ref, o_ref):
    rows = lax.broadcasted_iota(jnp.int32, (tab_ref.shape[0], ids_ref.shape[-1]), 0)
    hot = jnp.where(rows == ids_ref[0], 1.0, 0.0).astype(bf16)
    o_ref[0] = lax.dot_general(
        hot, tab_ref[...], (((0,), (0,)), ((), ())), preferred_element_type=f32
    ).astype(bf16)


def lookup(local_ids, table_low):
    count, tokens = local_ids.shape
    vocab = table_low.shape[0]
    return pl.pallas_call(
        lookup_kernel,
        grid=(count,),
        out_shape=jax.ShapeDtypeStruct((count, tokens, D), bf16),
        in_specs=[
            pl.BlockSpec((1, 1, tokens), lambda i: (i, 0, 0)),
            pl.BlockSpec((vocab, D), lambda i: (0, 0)),
        ],
        out_specs=pl.BlockSpec((1, tokens, D), lambda i: (i, 0, 0)),
        name="lookup",
    )(local_ids[:, None, :], table_low)


def spread_kernel(ids_ref, g_ref, base_ref, o_ref):
    rows = lax.broadcasted_iota(jnp.int32, (o_ref.shape[0], ids_ref.shape[-1]), 0)
    hot = jnp.where(rows == ids_ref[0], 1.0, 0.0).astype(bf16)

    @pl.when(pl.program_id(0) == 0)
    def _():
        o_ref[...] = base_ref[...]

    o_ref[...] += jnp.dot(hot, g_ref[0], preferred_element_type=f32)


def spread(local_ids, grads, base):
    count, tokens = local_ids.shape
    vocab = base.shape[0]
    return pl.pallas_call(
        spread_kernel,
        grid=(count,),
        out_shape=jax.ShapeDtypeStruct((vocab, D), f32),
        in_specs=[
            pl.BlockSpec((1, 1, tokens), lambda i: (i, 0, 0)),
            pl.BlockSpec((1, tokens, D), lambda i: (i, 0, 0)),
            pl.BlockSpec((vocab, D), lambda i: (0, 0)),
        ],
        out_specs=pl.BlockSpec((vocab, D), lambda i: (0, 0)),
        name="spread",
    )(local_ids[:, None, :], grads, base)


def stats_kernel(vocab, nf_ref, tab_ref, top_ref, sum_ref):
    logits = lax.dot_general(
        tab_ref[...], nf_ref[0], (((1,), (1,)), ((), ())), preferred_element_type=f32
    )
    rows = lax.broadcasted_iota(jnp.int32, logits.shape, 0)
    logits = jnp.where(rows < vocab, logits, -1e30)
    top = jnp.max(logits, axis=0, keepdims=True)
    top_ref[0] = top
    sum_ref[0] = jnp.sum(jnp.exp(logits - top), axis=0, keepdims=True)


def vocab_stats(normed, table_low, vocab):
    count, tokens, _ = normed.shape
    padded = table_low.shape[0]
    row = jax.ShapeDtypeStruct((count, 1, tokens), f32)
    return pl.pallas_call(
        functools.partial(stats_kernel, vocab),
        grid=(count,),
        out_shape=(row, row),
        in_specs=[
            pl.BlockSpec((1, tokens, D), lambda i: (i, 0, 0)),
            pl.BlockSpec((padded, D), lambda i: (0, 0)),
        ],
        out_specs=(
            pl.BlockSpec((1, 1, tokens), lambda i: (i, 0, 0)),
            pl.BlockSpec((1, 1, tokens), lambda i: (i, 0, 0)),
        ),
        name="vocab_stats",
    )(normed, table_low)


def vocab_kernel(vocab, scale, nf_ref, tab_ref, lse_ref, t0_ref, t1_ref, g_ref, acc_ref, pick_ref):
    logits = lax.dot_general(
        tab_ref[...], nf_ref[0], (((1,), (1,)), ((), ())), preferred_element_type=f32
    )
    rows = lax.broadcasted_iota(jnp.int32, logits.shape, 0)
    hits = jnp.where(rows == t0_ref[0], 1.0, 0.0) + jnp.where(rows == t1_ref[0], second_weight, 0.0)
    soft = jnp.exp(logits - lse_ref[0]) * (1.0 + second_weight)
    grad = jnp.where(rows < vocab, (soft - hits) * scale, 0.0).astype(bf16)

    @pl.when(pl.program_id(0) == 0)
    def _():
        acc_ref[...] = jnp.zeros_like(acc_ref)
        pick_ref[...] = jnp.zeros_like(pick_ref)

    pick_ref[...] += jnp.sum(hits * logits, axis=0, keepdims=True)
    g_ref[0] = lax.dot_general(
        grad, tab_ref[...], (((0,), (0,)), ((), ())), preferred_element_type=f32
    ).astype(bf16)
    acc_ref[...] += jnp.dot(grad, nf_ref[0], preferred_element_type=f32)


def vocab_grads(normed, table_low, log_total, first, second, vocab, scale):
    count, tokens, _ = normed.shape
    padded = table_low.shape[0]
    row = pl.BlockSpec((1, 1, tokens), lambda i: (i, 0, 0))
    return pl.pallas_call(
        functools.partial(vocab_kernel, vocab, scale),
        grid=(count,),
        out_shape=(
            jax.ShapeDtypeStruct((count, tokens, D), bf16),
            jax.ShapeDtypeStruct((padded, D), f32),
            jax.ShapeDtypeStruct((1, tokens), f32),
        ),
        in_specs=[
            pl.BlockSpec((1, tokens, D), lambda i: (i, 0, 0)),
            pl.BlockSpec((padded, D), lambda i: (0, 0)),
            row,
            row,
            row,
        ],
        out_specs=(
            pl.BlockSpec((1, tokens, D), lambda i: (i, 0, 0)),
            pl.BlockSpec((padded, D), lambda i: (0, 0)),
            pl.BlockSpec((1, tokens), lambda i: (0, 0)),
        ),
        name="vocab_grads",
    )(normed, table_low, log_total[:, None, :], first[:, None, :], second[:, None, :])


def place_of(index, shard):
    return (index % 2, index // (2 * shard), (index // 2) % shard)


def my_place():
    shard = lax.axis_size("shard")
    return (lax.axis_index("blk") * shard + lax.axis_index("shard")) * 2 + lax.axis_index("section")


def meet(reach, block, blocks, mine, shard, sign):
    barrier = pltpu.get_barrier_semaphore()
    above = [block + d < blocks for d in range(1, reach + 1)]
    below = [block >= d for d in range(1, reach + 1)]
    sources, targets = (below, above) if sign > 0 else (above, below)
    for d in range(1, reach + 1):

        @pl.when(sources[d - 1])
        def _():
            pl.semaphore_signal(
                barrier, inc=1, device_id=place_of(mine - sign * d, shard), device_id_type=MESH
            )

    @pl.when(targets[0])
    def _():
        pl.semaphore_wait(barrier, sum(held.astype(jnp.int32) for held in targets))


def half_masks(tokens):
    lane = lax.broadcasted_iota(jnp.int32, (tokens, 2 * HEAD_DIM), 1)
    return lane < HEAD_DIM


def allowed_mask(d, seg_ref, tokens):
    own = jnp.transpose(jnp.broadcast_to(seg_ref[0], (128, tokens)))[:, :1]
    allowed = own == seg_ref[d]
    if d == 0:
        row = lax.broadcasted_iota(jnp.int32, (tokens, tokens), 0)
        col = lax.broadcasted_iota(jnp.int32, (tokens, tokens), 1)
        allowed = allowed & (col <= row)
    return allowed


def attend_kernel(reach, blocks, q_ref, k_ref, v_ref, seg_ref, tot_ref, acc_ref, kr_ref, vr_ref,
                  send_sem, recv_sem):
    shard = lax.axis_size("shard")
    mine = (lax.axis_index("blk") * shard + lax.axis_index("shard")) * 2 + lax.axis_index("section")
    block = mine % blocks
    tokens = q_ref.shape[0]
    meet(reach, block, blocks, mine, shard, 1)

    def copies(d):
        target = place_of(mine + d, shard)
        return [
            pltpu.make_async_remote_copy(
                src_ref=source,
                dst_ref=target_ref.at[d - 1],
                send_sem=send_sem.at[d - 1, i],
                recv_sem=recv_sem.at[d - 1, i],
                device_id=target,
                device_id_type=MESH,
            )
            for i, (source, target_ref) in enumerate(((k_ref, kr_ref), (v_ref, vr_ref)))
        ]

    for d in range(reach, 0, -1):

        @pl.when(block + d < blocks)
        def _():
            for copy in copies(d):
                copy.start()

    scale = HEAD_DIM ** (-0.5)
    left = half_masks(tokens)
    zero = jnp.zeros((tokens, 2 * HEAD_DIM), bf16)

    def visit(d, keys, values):
        allowed = allowed_mask(d, seg_ref, tokens)

        @pl.loop(0, HEADS // 2)
        def _(pair):
            lanes = pl.ds(pl.multiple_of(pair * 128, 128), 128)
            q_pair, k_pair, v_pair = q_ref[:, lanes], keys[:, lanes], values[:, lanes]
            totals, sums = [], []
            for side in (left, ~left):
                scores = lax.dot_general(
                    jnp.where(side, q_pair, zero),
                    k_pair,
                    (((1,), (1,)), ((), ())),
                    preferred_element_type=f32,
                )
                expo = jnp.where(allowed, jnp.exp(scores * scale), 0.0)
                totals.append(jnp.sum(expo, axis=1, keepdims=True))
                sums.append(jnp.dot(expo.astype(bf16), v_pair, preferred_element_type=f32))
            total = jnp.where(left, totals[0], totals[1])
            added = jnp.where(left, sums[0], sums[1])
            if d == 0:
                tot_ref[:, lanes] = total
                acc_ref[:, lanes] = added
            else:
                tot_ref[:, lanes] += total
                acc_ref[:, lanes] += added

    visit(0, k_ref, v_ref)
    for d in range(1, reach + 1):

        @pl.when(block >= d)
        def _():
            for copy in copies(d):
                copy.wait_recv()
            visit(d, kr_ref.at[d - 1], vr_ref.at[d - 1])

    for d in range(1, reach + 1):

        @pl.when(block + d < blocks)
        def _():
            for copy in copies(d):
                copy.wait_send()


def attend(q, k, v, seg_rows, reach, blocks, cid):
    tokens = q.shape[0]
    wide = jax.ShapeDtypeStruct((tokens, D), f32)
    far = jax.ShapeDtypeStruct((reach, tokens, D), bf16)
    whole = pl.BlockSpec(memory_space=pltpu.VMEM)
    return pl.pallas_call(
        functools.partial(attend_kernel, reach, blocks),
        out_shape=(wide, wide, far, far),
        in_specs=[whole] * 4,
        out_specs=(whole,) * 4,
        scratch_shapes=[
            pltpu.SemaphoreType.DMA((reach, 2)),
            pltpu.SemaphoreType.DMA((reach, 2)),
        ],
        compiler_params=pltpu.CompilerParams(
            collective_id=cid, has_side_effects=True, vmem_limit_bytes=VMEM_MAX
        ),
        name="attend",
    )(q, k, v, seg_rows)


def attend_back_kernel(reach, blocks, q_ref, k_ref, v_ref, kr_ref, vr_ref, tot_ref, acc_ref, ga_ref,
                       seg_ref, dq_ref, dk_ref, dv_ref, gw, gt, far_k, far_v, got_k, got_v,
                       send_sem, recv_sem):
    shard = lax.axis_size("shard")
    mine = (lax.axis_index("blk") * shard + lax.axis_index("shard")) * 2 + lax.axis_index("section")
    block = mine % blocks
    tokens = q_ref.shape[0]
    meet(reach, block, blocks, mine, shard, -1)
    scale = HEAD_DIM ** (-0.5)
    left = half_masks(tokens)
    zero = jnp.zeros((tokens, 2 * HEAD_DIM), bf16)

    @pl.loop(0, HEADS // 2)
    def _(pair):
        lanes = pl.ds(pl.multiple_of(pair * 128, 128), 128)
        inverse = 1.0 / tot_ref[:, lanes]
        grad = ga_ref[:, lanes]
        gw[:, lanes] = (grad * inverse).astype(bf16)
        product = grad * acc_ref[:, lanes]
        first = jnp.sum(jnp.where(left, product, 0.0), axis=1, keepdims=True)
        second = jnp.sum(jnp.where(left, 0.0, product), axis=1, keepdims=True)
        gt[:, lanes] = -jnp.where(left, first, second) * inverse * inverse
        dq_ref[:, lanes] = jnp.zeros((tokens, 128), f32)

    def visit(d, keys, values, out_k, out_v):
        allowed = allowed_mask(d, seg_ref, tokens)

        @pl.loop(0, HEADS // 2)
        def _(pair):
            lanes = pl.ds(pl.multiple_of(pair * 128, 128), 128)
            q_pair, k_pair, v_pair, w_pair = q_ref[:, lanes], keys[:, lanes], values[:, lanes], gw[:, lanes]
            gt_pair = gt[:, lanes]
            dq, dk, dv = [], [], []
            for i, side in enumerate((left, ~left)):
                scores = lax.dot_general(
                    jnp.where(side, q_pair, zero),
                    k_pair,
                    (((1,), (1,)), ((), ())),
                    preferred_element_type=f32,
                )
                expo = jnp.where(allowed, jnp.exp(scores * scale), 0.0)
                probs = lax.dot_general(
                    jnp.where(side, w_pair, zero),
                    v_pair,
                    (((1,), (1,)), ((), ())),
                    preferred_element_type=f32,
                )
                part = (expo * (probs + gt_pair[:, i * HEAD_DIM : i * HEAD_DIM + 1])).astype(bf16)
                dq.append(jnp.dot(part, k_pair, preferred_element_type=f32))
                dk.append(
                    lax.dot_general(part, q_pair, (((0,), (0,)), ((), ())), preferred_element_type=f32)
                )
                dv.append(
                    lax.dot_general(
                        expo.astype(bf16), w_pair, (((0,), (0,)), ((), ())), preferred_element_type=f32
                    )
                )
            dq_ref[:, lanes] += jnp.where(left, dq[0], dq[1]) * scale
            out_k[:, lanes] = (jnp.where(left, dk[0], dk[1]) * scale).astype(out_k.dtype)
            out_v[:, lanes] = jnp.where(left, dv[0], dv[1]).astype(out_v.dtype)

    def copies(d):
        target = place_of(mine - d, shard)
        return [
            pltpu.make_async_remote_copy(
                src_ref=source.at[d - 1],
                dst_ref=target_ref.at[d - 1],
                send_sem=send_sem.at[d - 1, i],
                recv_sem=recv_sem.at[d - 1, i],
                device_id=target,
                device_id_type=MESH,
            )
            for i, (source, target_ref) in enumerate(((far_k, got_k), (far_v, got_v)))
        ]

    for d in range(reach, 0, -1):

        @pl.when(block >= d)
        def _():
            visit(d, kr_ref.at[d - 1], vr_ref.at[d - 1], far_k.at[d - 1], far_v.at[d - 1])
            for copy in copies(d):
                copy.start()

    visit(0, k_ref, v_ref, dk_ref, dv_ref)
    for d in range(reach, 0, -1):

        @pl.when(block + d < blocks)
        def _():
            for copy in copies(d):
                copy.wait_recv()
            dk_ref[...] += got_k[d - 1].astype(f32)
            dv_ref[...] += got_v[d - 1].astype(f32)

    for d in range(1, reach + 1):

        @pl.when(block >= d)
        def _():
            for copy in copies(d):
                copy.wait_send()


def attend_back(q, k, v, far_k, far_v, total, accum, grad, seg_rows, reach, blocks, cid):
    tokens = q.shape[0]
    wide = jax.ShapeDtypeStruct((tokens, D), f32)
    whole = pl.BlockSpec(memory_space=pltpu.VMEM)
    return pl.pallas_call(
        functools.partial(attend_back_kernel, reach, blocks),
        out_shape=(wide, wide, wide),
        in_specs=[whole] * 9,
        out_specs=(whole,) * 3,
        scratch_shapes=[pltpu.VMEM((tokens, D), bf16), pltpu.VMEM((tokens, D), f32)]
        + [pltpu.VMEM((reach, tokens, D), bf16)] * 4
        + [pltpu.SemaphoreType.DMA((reach, 2)), pltpu.SemaphoreType.DMA((reach, 2))],
        compiler_params=pltpu.CompilerParams(
            collective_id=cid, has_side_effects=True, vmem_limit_bytes=VMEM_MAX
        ),
        name="attend_back",
    )(q, k, v, far_k, far_v, total, accum, grad, seg_rows)


def matrix_layout():
    return ((D, 3 * D), (D, D), (D, 2 * FF), (FF, D))


def blocks_to_rows(blocks):
    count = blocks.shape[0]
    if count % 4:
        return blocks.reshape(-1, QUAD)
    quads = blocks.reshape(count // 4, 4, BS, BS).transpose(0, 2, 1, 3)
    return quads.reshape(-1, QUAD)


def rows_to_blocks(rows):
    count = rows.shape[0] * QUAD // (BS * BS)
    if count % 4:
        return rows.reshape(count, BS, BS)
    return rows.reshape(count // 4, BS, 4, BS).transpose(0, 2, 1, 3).reshape(count, BS, BS)


def rows_to_quads(rows, count):
    if count % 4:
        rows = rows.reshape(-1, 4, BS, BS).transpose(0, 2, 1, 3)
    return rows.reshape(-1, BS, QUAD)


def quads_to_rows(quads, count):
    if count % 4:
        quads = quads.reshape(-1, BS, 4, BS).transpose(0, 2, 1, 3)
    return quads.reshape(-1, count * BS * BS // QUAD, QUAD)


def rope_tables(positions):
    half_dim = HEAD_DIM // 2
    frequency = rope_base ** (-jnp.arange(half_dim, dtype=f32) * 2.0 / HEAD_DIM)
    angles = positions.astype(f32)[:, None] * frequency[None, :]
    cosine, sine = jnp.cos(angles), jnp.sin(angles)
    return (
        jnp.concatenate([cosine, cosine] * 4, axis=-1),
        jnp.concatenate([-sine, sine] * 4, axis=-1),
    )


QKV, OUT, GATE, DOWN = (0, 12, 9), (108, 12, 3), (144, 12, 16), (336, 32, 3)
QUADS = 432
WHOLE = pl.BlockSpec(memory_space=pltpu.VMEM)
LEFT = pl.BlockSpec(memory_space=pl.ANY)


def struct(shape, dtype=f32):
    return jax.ShapeDtypeStruct(shape, dtype)


def column(buf, kind, c, base=0):
    offset, rows, cols = kind
    return jnp.concatenate([buf[offset - base + r * cols + c] for r in range(rows)], axis=0)


def band(buf, kind, r, base=0):
    offset, _, cols = kind
    return jnp.concatenate(
        [
            jnp.concatenate([buf[offset - base + (4 * r + i) * cols + c] for c in range(cols)], axis=1)
            for i in range(4)
        ],
        axis=0,
    )


def lanes_of(c):
    return pl.ds(pl.multiple_of(c * QUAD, QUAD), QUAD)


def dot(left_side, right_side):
    return jnp.dot(left_side, right_side, preferred_element_type=f32)


def dot_nt(left_side, right_side):
    return lax.dot_general(
        left_side, right_side, (((1,), (1,)), ((), ())), preferred_element_type=f32
    )


def norm_of(x):
    return lax.rsqrt(jnp.mean(x * x, axis=-1, keepdims=True) + norm_eps)


def norm_back(x, gain, grad):
    inverse = norm_of(x)
    weighted = grad * gain
    grad_in = inverse * weighted - x * (inverse * inverse * inverse) * jnp.mean(
        weighted * x, axis=-1, keepdims=True
    )
    return grad_in, jnp.sum(grad * x * inverse, axis=0, keepdims=True)


def swapped(u):
    lane = lax.broadcasted_iota(jnp.int32, u.shape, 1)
    half = HEAD_DIM // 2
    return jnp.where(
        lane % HEAD_DIM < half, pltpu.roll(u, u.shape[1] - half, 1), pltpu.roll(u, half, 1)
    )


def load_quads(w_ref, layer, kinds, bufs, sem):
    copies = []
    for i, ((offset, rows, cols), buf) in enumerate(zip(kinds, bufs)):
        copy = pltpu.make_async_copy(w_ref.at[layer, pl.ds(offset, rows * cols)], buf, sem.at[i])
        copy.start()
        copies.append(copy)
    return copies


def quad_buffers(kinds):
    return [pltpu.VMEM((rows * cols, BS, QUAD), bf16) for _, rows, cols in kinds] + [
        pltpu.SemaphoreType.DMA((len(kinds),))
    ]


def big(**extra):
    return pltpu.CompilerParams(vmem_limit_bytes=VMEM_MAX, **extra)


def qkv_kernel(layer, x_ref, gain_ref, cos_ref, sin_ref, w_ref, a_ref, q_ref, k_ref, v_ref, wq, sem):
    (copy,) = load_quads(w_ref, layer, (QKV,), (wq,), sem)
    x = x_ref[...]
    a_ref[...] = (x * norm_of(x) * gain_ref[...]).astype(bf16)
    copy.wait()
    for i, out in enumerate((q_ref, k_ref, v_ref)):

        @pl.loop(0, 3)
        def _(c):
            part = dot(a_ref[...], column(wq, QKV, 3 * i + c, QKV[0]))
            if i < 2:
                part = part * cos_ref[...] + swapped(part) * sin_ref[...]
            out[:, lanes_of(c)] = part.astype(bf16)


def qkv_forward(layer, x, gain, cosine, sine, quads):
    tokens = x.shape[0]
    low = struct((tokens, D), bf16)
    return pl.pallas_call(
        functools.partial(qkv_kernel, layer),
        out_shape=(low,) * 4,
        in_specs=[WHOLE] * 4 + [LEFT],
        out_specs=(WHOLE,) * 4,
        scratch_shapes=quad_buffers((QKV,)),
        compiler_params=big(),
        name="qkv",
    )(x, gain, cosine, sine, quads)


def mlp_kernel(layer, last, x_ref, acc_ref, tot_ref, gain_ref, final_ref, w_ref, out_ref, att_ref,
               mixed_ref, nm_ref, gate_ref, up_ref, hid_ref, nf_ref, wo, wg, wd, sem):
    copies = load_quads(w_ref, layer, (OUT, GATE, DOWN), (wo, wg, wd), sem)
    att_ref[...] = (acc_ref[...] / tot_ref[...]).astype(bf16)
    copies[0].wait()

    @pl.loop(0, 3)
    def _(c):
        lanes = lanes_of(c)
        mixed_ref[:, lanes] = x_ref[:, lanes] + dot(att_ref[...], column(wo, OUT, c, OUT[0]))

    mixed = mixed_ref[...]
    nm_ref[...] = (mixed * norm_of(mixed) * gain_ref[...]).astype(bf16)
    copies[1].wait()

    @pl.loop(0, FF // QUAD)
    def _(c):
        lanes = lanes_of(c)
        gate = dot(nm_ref[...], column(wg, GATE, c, GATE[0]))
        upper = dot(nm_ref[...], column(wg, GATE, c + FF // QUAD, GATE[0]))
        gate_ref[:, lanes] = gate
        up_ref[:, lanes] = upper
        hid_ref[:, lanes] = (gate / (1.0 + jnp.exp(-gate)) * upper).astype(bf16)

    copies[2].wait()

    @pl.loop(0, 3)
    def _(c):
        lanes = lanes_of(c)
        out_ref[:, lanes] = mixed_ref[:, lanes] + dot(hid_ref[...], column(wd, DOWN, c, DOWN[0]))

    if last:
        out = out_ref[...]
        nf_ref[...] = (out * norm_of(out) * final_ref[...]).astype(bf16)
    else:
        nf_ref[...] = jnp.zeros_like(nf_ref)


def mlp_forward(layer, last, x, accum, total, gain, final_gain, quads):
    tokens = x.shape[0]
    wide, low = struct((tokens, D)), struct((tokens, D), bf16)
    return pl.pallas_call(
        functools.partial(mlp_kernel, layer, last),
        out_shape=(
            wide, low, wide, low, struct((tokens, FF)), struct((tokens, FF)),
            struct((tokens, FF), bf16), low,
        ),
        in_specs=[WHOLE] * 5 + [LEFT],
        out_specs=(WHOLE,) * 8,
        scratch_shapes=quad_buffers((OUT, GATE, DOWN)),
        compiler_params=big(),
        name="mlp",
    )(x, accum, total, gain, final_gain, quads)


def put_quads(buf, kind, c, value, base):
    offset, rows, cols = kind
    for r in range(rows):
        buf[offset - base + r * cols + c] = value[r * BS : (r + 1) * BS].astype(bf16)


def mlp_back_kernel(layer, last, first_call, *refs):
    (gy_ref, h_ref, mixed_ref, nm_ref, gate_ref, up_ref, hid_ref, att_ref, gain_ref, final_ref,
     w_ref) = refs[:11]
    (p_ref, gm_ref, gatt_ref, gg_ref, gf_ref, wo, wg, wd, sem, grads, gl, ggu, turned, gin,
     out_sem) = refs[11 + (not first_call):]
    copies = load_quads(w_ref, layer, (DOWN, GATE, OUT), (wd, wg, wo), sem)
    base = OUT[0]
    if last:
        grad, gain_row = norm_back(h_ref[...], final_ref[...], gy_ref[...].astype(f32))
        gf_ref[...] = gain_row
    else:
        grad = gy_ref[...]
        gf_ref[...] = jnp.zeros_like(gf_ref)
    gin[...] = grad
    gl[...] = grad.astype(bf16)
    copies[0].wait()

    @pl.loop(0, FF // QUAD)
    def _(r):
        lanes = lanes_of(r)
        grad_down = dot(jnp.transpose(hid_ref[:, lanes]), gl[...])
        for i in range(4):
            for c in range(3):
                grads[DOWN[0] - base + (4 * r + i) * 3 + c] = grad_down[
                    i * BS : (i + 1) * BS, c * QUAD : (c + 1) * QUAD
                ].astype(bf16)
        grad_hidden = dot_nt(gl[...], band(wd, DOWN, r, DOWN[0]))
        gate, upper = gate_ref[:, lanes], up_ref[:, lanes]
        sig = 1.0 / (1.0 + jnp.exp(-gate))
        ggu[:, lanes] = (grad_hidden * upper * sig * (1.0 + gate * (1.0 - sig))).astype(bf16)
        ggu[:, lanes_of(r + FF // QUAD)] = (grad_hidden * gate * sig).astype(bf16)

    def send(i, kind):
        offset, rows, cols = kind
        copy = pltpu.make_async_copy(
            grads.at[pl.ds(offset - base, rows * cols)],
            p_ref.at[layer, pl.ds(offset, rows * cols)],
            out_sem.at[i],
        )
        copy.start()
        return copy

    sent = [send(0, DOWN)]
    turned[...] = jnp.transpose(nm_ref[...])
    gatt_ref[...] = jnp.zeros_like(gatt_ref)
    copies[1].wait()

    @pl.loop(0, 2 * FF // QUAD)
    def _(c):
        part = ggu[:, lanes_of(c)]
        put_quads(grads, GATE, c, dot(turned[...], part), base)
        gatt_ref[...] += dot_nt(part, column(wg, GATE, c, GATE[0]))

    sent.append(send(1, GATE))
    grad_norm, gain_row = norm_back(mixed_ref[...], gain_ref[...], gatt_ref[...])
    gg_ref[...] = gain_row
    grad_mixed = gin[...] + grad_norm
    gm_ref[...] = grad_mixed
    gl[...] = grad_mixed.astype(bf16)
    turned[...] = jnp.transpose(att_ref[...])
    gatt_ref[...] = jnp.zeros_like(gatt_ref)
    copies[2].wait()

    @pl.loop(0, 3)
    def _(c):
        part = gl[:, lanes_of(c)]
        put_quads(grads, OUT, c, dot(turned[...], part), base)
        gatt_ref[...] += dot_nt(part, column(wo, OUT, c, OUT[0]))

    sent.append(send(2, OUT))
    for copy in sent:
        copy.wait()


def mlp_backward(layer, last, grad, states, cache, gain, final_gain, quads, store):
    mixed, nm, gate, upper, hidden, att = cache
    tokens = mixed.shape[0]
    wide, row = struct((tokens, D)), struct((1, D))
    kinds = (DOWN, GATE, OUT)
    buffers = quad_buffers((OUT, GATE, DOWN))
    operands = [grad, states, mixed, nm, gate, upper, hidden, att, gain, final_gain, quads]
    aliases = {}
    if store is not None:
        operands.append(store)
        aliases = {11: 0}
    return pl.pallas_call(
        functools.partial(mlp_back_kernel, layer, last, store is None),
        out_shape=(struct((2, QUADS, BS, QUAD), bf16), wide, wide, row, row),
        in_specs=[WHOLE] * 10 + [LEFT] * (len(operands) - 10),
        out_specs=(LEFT,) + (WHOLE,) * 4,
        scratch_shapes=buffers
        + [
            pltpu.VMEM((QUADS - OUT[0], BS, QUAD), bf16),
            pltpu.VMEM((tokens, D), bf16),
            pltpu.VMEM((tokens, 2 * FF), bf16),
            pltpu.VMEM((D, tokens), bf16),
            pltpu.VMEM((tokens, D), f32),
            pltpu.SemaphoreType.DMA((3,)),
        ],
        input_output_aliases=aliases,
        compiler_params=big(),
        name="mlp_back",
    )(*operands)


def qkv_back_kernel(layer, dq_ref, dk_ref, dv_ref, a_ref, x_ref, gm_ref, gain_ref, cos_ref, sin_ref,
                    w_ref, store_ref, p_ref, gx_ref, low_ref, gg_ref, wq, sem, grads, turned, out_sem):
    (copy,) = load_quads(w_ref, layer, (QKV,), (wq,), sem)
    turned[...] = jnp.transpose(a_ref[...])
    gx_ref[...] = jnp.zeros_like(gx_ref)
    copy.wait()
    for i, ref in enumerate((dq_ref, dk_ref, dv_ref)):

        @pl.loop(0, 3)
        def _(c):
            part = ref[:, lanes_of(c)]
            if i < 2:
                part = part * cos_ref[...] - swapped(part) * sin_ref[...]
            part = part.astype(bf16)
            put_quads(grads, QKV, 3 * i + c, dot(turned[...], part), QKV[0])
            gx_ref[...] += dot_nt(part, column(wq, QKV, 3 * i + c, QKV[0]))

    out = pltpu.make_async_copy(
        grads, p_ref.at[layer, pl.ds(QKV[0], QKV[1] * QKV[2])], out_sem.at[0]
    )
    out.start()
    grad_norm, gain_row = norm_back(x_ref[...], gain_ref[...], gx_ref[...])
    gg_ref[...] = gain_row
    grad = gm_ref[...] + grad_norm
    gx_ref[...] = grad
    low_ref[...] = grad.astype(bf16)
    out.wait()


def qkv_backward(layer, dq, dk, dv, a, x, grad_mixed, gain, cosine, sine, quads, store):
    tokens = x.shape[0]
    return pl.pallas_call(
        functools.partial(qkv_back_kernel, layer),
        out_shape=(
            struct((2, QUADS, BS, QUAD), bf16), struct((tokens, D)), struct((tokens, D), bf16),
            struct((1, D)),
        ),
        in_specs=[WHOLE] * 9 + [LEFT] * 2,
        out_specs=(LEFT,) + (WHOLE,) * 3,
        scratch_shapes=quad_buffers((QKV,))
        + [
            pltpu.VMEM((QKV[1] * QKV[2], BS, QUAD), bf16),
            pltpu.VMEM((D, tokens), bf16),
            pltpu.SemaphoreType.DMA((1,)),
        ],
        input_output_aliases={10: 0},
        compiler_params=big(),
        name="qkv_back",
    )(dq, dk, dv, a, x, grad_mixed, gain, cosine, sine, quads, store)


def shampoo_kernel(scale_ref, g_ref, w_ref, ls_ref, rs_ref, lr_ref, rr_ref, wn_ref, wl_ref, ln_ref,
                   rn_ref):
    factor = scale_ref[0, 0]
    row = lax.broadcasted_iota(jnp.int32, (QUAD, QUAD), 0)
    col = lax.broadcasted_iota(jnp.int32, (QUAD, QUAD), 1)
    same = (row // BS) == (col // BS)

    def diagonal(wide):
        return jnp.where(same, jnp.concatenate([wide] * 4, axis=0), jnp.zeros((), wide.dtype))

    for j in range(g_ref.shape[0]):

        def side(ref):
            return jnp.concatenate([ref[4 * j + i] for i in range(4)], axis=1).astype(bf16)

        g = g_ref[j]
        left = dot_nt(g, diagonal(g)) * (factor * factor * (1.0 - stat_decay))
        right = lax.dot_general(g, g, (((0,), (0,)), ((), ())), preferred_element_type=f32)
        right = right * (factor * factor * (1.0 - stat_decay))
        inner = dot(g, diagonal(side(rr_ref))) * factor
        step = dot(side(lr_ref), diagonal(inner.astype(bf16)))
        for i in range(4):
            cut = slice(i * BS, (i + 1) * BS)
            n = 4 * j + i
            ln_ref[n] = stat_decay * ls_ref[n] + left[:, cut]
            rn_ref[n] = stat_decay * rs_ref[n] + right[cut, cut]
            new = w_ref[n] - shampoo_rate * step[:, cut]
            wn_ref[n] = new
            wl_ref[n] = new.astype(bf16)


def shampoo(factor, rows, weights, left_stats, right_stats, left_root, right_root):
    count = weights.shape[0]
    quads = 3
    square = pl.BlockSpec((4 * quads, BS, BS), lambda i: (i, 0, 0))
    return pl.pallas_call(
        shampoo_kernel,
        grid=(count // (4 * quads),),
        out_shape=(
            struct((count, BS, BS)), struct((count, BS, BS), bf16), struct((count, BS, BS)),
            struct((count, BS, BS)),
        ),
        in_specs=[
            pl.BlockSpec(memory_space=pltpu.SMEM),
            pl.BlockSpec((quads, BS, QUAD), lambda i: (i, 0, 0)),
        ]
        + [square] * 5,
        out_specs=(square,) * 4,
        name="shampoo",
    )(
        factor.reshape(1, 1), rows.reshape(-1, BS, QUAD), weights, left_stats, right_stats,
        left_root, right_root,
    )


def shampoo_plain(factor, rows, weights, left_stats, right_stats, left_root, right_root):
    grads = rows_to_blocks(rows.astype(f32)) * factor
    left_new = stat_decay * left_stats + (1.0 - stat_decay) * jnp.einsum(
        "bij,bkj->bik", grads, grads, precision=highest
    )
    right_new = stat_decay * right_stats + (1.0 - stat_decay) * jnp.einsum(
        "bji,bjk->bik", grads, grads, precision=highest
    )
    direction = jnp.einsum(
        "bij,bjk->bik",
        left_root,
        jnp.einsum("bij,bjk->bik", grads, right_root, precision=highest),
        precision=highest,
    )
    new = weights - shampoo_rate * direction
    return new, new.astype(bf16), left_new, right_new


def adam_step(weight, first, second, grad_in, decay):
    first_new = beta_first * first + (1.0 - beta_first) * grad_in
    second_new = beta_second * second + (1.0 - beta_second) * grad_in * grad_in
    weight_new = weight - adam_rate * (
        first_new / (jnp.sqrt(second_new) + adam_eps) + decay * weight
    )
    return (weight_new, first_new, second_new)


def share_ids(packed, cid):
    blk, shard = lax.axis_size("blk"), lax.axis_size("shard")
    if blk * shard <= 16:
        every = swap_all(packed, 2 * blk * shard, cid, name="swap_ids")
        return every.reshape(blk, shard, 2, *packed.shape)[:, :, 0]
    return lax.all_gather(packed, ("blk", "shard")).reshape(blk, shard, *packed.shape)


def share_stats(top, total, cid):
    blk, shard = lax.axis_size("blk"), lax.axis_size("shard")
    devices = 2 * blk * shard
    if blk * shard <= 16:
        pair = jnp.concatenate([top, total], axis=1)
        return swap_all(pair, devices, cid, join_stats, 1, name="swap_stats")[:, 0]
    largest = lax.pmax(top[:, 0], ORDER)
    return largest + jnp.log(lax.psum(total[:, 0] * jnp.exp(top[:, 0] - largest), ORDER))


def share_sum(small, cid):
    blk, shard = lax.axis_size("blk"), lax.axis_size("shard")
    devices = 2 * blk * shard
    if blk * shard <= 16:
        lanes = pl.cdiv(small.size, devices * 128) * 128
        flat = jnp.pad(small.reshape(-1), (0, devices * lanes - small.size))
        every = swap_all(flat.reshape(devices, 1, lanes), devices, cid, join_sum, 1, name="swap_sum")
        return every.reshape(-1)[: small.size].reshape(small.shape)
    return lax.psum(small, ORDER)


def on_device(ids, targets, segments, table, table_m, table_v, blocks, left_stats, right_stats,
              left_root, right_root, gains, gains_m, gains_v):
    blk, shard = lax.axis_size("blk"), lax.axis_size("shard")
    section = lax.axis_index("section")
    blk_index, shard_index = lax.axis_index("blk"), lax.axis_index("shard")
    devices = 2 * blk * shard
    micro, _, tok_rows = ids.shape
    seq_len = segments.shape[2]
    all_tokens = micro * shard * seq_len
    tokens = all_tokens // devices
    seq_blocks = seq_len // tokens
    reach = pl.cdiv(seq_len // 2 - 1, tokens)
    vocab = table.shape[0]
    padded = pl.cdiv(vocab, 128) * 128
    own_blocks = blocks.shape[1]

    mine = my_place()
    seg_own = lax.dynamic_slice_in_dim(segments[:, 0, :], blk_index * tok_rows, tok_rows, axis=1)
    packed = jnp.stack(
        [ids[:, 0, :], targets[:, 0, :, 0], targets[:, 0, :, 1], seg_own], axis=0
    ).reshape(4 * micro, tok_rows)
    shared = share_ids(packed, 8).reshape(blk, shard, 4, micro, tok_rows)
    shared = shared.transpose(2, 3, 1, 0, 4).reshape(4, devices, tokens)
    first_row = ((section * blk + blk_index) * shard + shard_index) * vocab
    local_ids, local_first, local_second = (shared[i] - first_row for i in range(3))

    def mark(values):
        return jnp.where((values >= 0) & (values < vocab), values, -1)

    local_ids, local_first, local_second = mark(local_ids), mark(local_first), mark(local_second)
    seg_index = jnp.maximum(mine - jnp.arange(reach + 1), 0)
    seg_rows = jnp.take(shared[3], seg_index, axis=0).astype(f32)[:, None, :]

    rows_low = blocks_to_rows(blocks[0].astype(bf16))
    gathered = gather_all(rows_low, 0, by_section=True)
    weights = jnp.stack([rows_to_quads(part, own_blocks) for part in gathered.reshape(
        2, blk * shard * rows_low.shape[0], QUAD)]) if own_blocks % 4 else gathered.reshape(
        2, QUADS, BS, QUAD)
    table_low = jnp.pad(table.astype(bf16), ((0, padded - vocab), (0, 0)))
    looked = lookup(local_ids, table_low)
    states = scatter_all(looked, 1).astype(f32)

    positions = (mine % seq_blocks) * tokens + jnp.arange(tokens, dtype=jnp.int32)
    cosine, sine = rope_tables(positions)
    rows_of_gain = [gains[i : i + 1] for i in range(5)]
    caches = []
    for l in range(2):
        a, q, k, v = qkv_forward(l, states, rows_of_gain[2 * l], cosine, sine, weights)
        total, accum, far_k, far_v = attend(q, k, v, seg_rows, reach, seq_blocks, 2)
        out, att, mixed, nm, gate, upper, hidden, normed_own = mlp_forward(
            l, l == 1, states, accum, total, rows_of_gain[2 * l + 1], rows_of_gain[4], weights
        )
        caches.append(
            (states, a, q, k, v, far_k, far_v, total, accum, (mixed, nm, gate, upper, hidden, att))
        )
        states = out
    normed = gather_all(normed_own, 3)
    top, spread_sum = vocab_stats(normed, table_low, vocab)
    log_total = share_stats(top, spread_sum, 4)
    inv_count = 1.0 / all_tokens
    grad_rows, head_term, picks = vocab_grads(
        normed, table_low, log_total, local_first, local_second, vocab, inv_count
    )
    own_log = lax.dynamic_index_in_dim(log_total, mine, 0, keepdims=False)
    loss_part = (1.0 + second_weight) * jnp.sum(own_log) - jnp.sum(picks)
    grad = scatter_all(grad_rows, 1)
    gain_grads = [None] * 5
    store = None
    for l in (1, 0):
        before, a, q, k, v, far_k, far_v, total, accum, cache = caches[l]
        store, grad_mixed, grad_att, gain_grads[2 * l + 1], final_row = mlp_backward(
            l, l == 1, grad, states, cache, rows_of_gain[2 * l + 1], rows_of_gain[4], weights, store
        )
        if l == 1:
            gain_grads[4] = final_row
        dq, dk, dv = attend_back(
            q, k, v, far_k, far_v, total, accum, grad_att, seg_rows, reach, seq_blocks, 5
        )
        store, grad, grad_low, gain_grads[2 * l] = qkv_backward(
            l, dq, dk, dv, a, before, grad_mixed, rows_of_gain[2 * l], cosine, sine, weights, store
        )
    sends = store
    if own_blocks % 4:
        sends = jnp.stack([quads_to_rows(store[l], own_blocks) for l in range(2)])
    sends = sends.reshape(devices, rows_low.shape[0], QUAD)
    block_rows = scatter_all(sends, 6, by_section=True)
    grad_embed = gather_all(grad_low, 3)
    table_own = spread(local_ids, grad_embed, head_term)[:vocab]
    square_rows = block_rows.astype(f32)
    square_sum = jnp.sum(table_own * table_own) + jnp.sum(square_rows * square_rows)
    small = jnp.concatenate(
        gain_grads
        + [jnp.full((1, D), square_sum), jnp.full((1, D), loss_part), jnp.zeros((1, D), f32)]
    )
    summed = share_sum(small, 7)
    gain_grad = summed[:5]
    clip_norm = jnp.sqrt(summed[5, 0] + jnp.sum(gain_grad * gain_grad))
    factor = clip_bound / jnp.maximum(clip_norm, clip_bound)
    loss = summed[6, 0] * inv_count
    update = shampoo if own_blocks % 12 == 0 else shampoo_plain
    blocks_new, blocks_low, left_new, right_new = update(
        factor, block_rows, blocks[0], left_stats[0], right_stats[0], left_root[0], right_root[0]
    )
    table_new, table_m_new, table_v_new = adam_step(
        table, table_m, table_v, table_own * factor, weight_decay
    )
    gains_new, gains_m_new, gains_v_new = adam_step(
        gains, gains_m, gains_v, gain_grad * factor, 0.0
    )
    return (
        loss, clip_norm, table_new, table_m_new, table_v_new, table_new.astype(bf16),
        blocks_new[None], blocks_low[None], left_new[None], right_new[None],
        gains_new, gains_m_new, gains_v_new,
    )


def solution(mesh):
    rows = P(("section", "blk", "shard"), None)
    square = P("section", ("blk", "shard"), None, None)
    return jax.shard_map(
        on_device,
        mesh=mesh,
        in_specs=(
            P(None, "shard", "blk"),
            P(None, "shard", "blk", None),
            P(None, "shard", None),
            rows, rows, rows,
            square, square, square, square, square,
            P(), P(), P(),
        ),
        out_specs=(
            P(), P(),
            rows, rows, rows, rows,
            square, square, square, square,
            P(), P(), P(),
        ),
        check_vma=False,
    )
```

```python
import functools

import jax
import jax.numpy as jnp
from jax import lax
from jax.experimental import pallas as pl
from jax.experimental.pallas import tpu as pltpu
from jax.sharding import PartitionSpec as P

D = 768
HEADS = 12
HEAD_DIM = 64
FF = 2048
BS = 64
QUAD = 256

norm_eps = 1e-05
rope_base = 10000.0
clip_bound = 0.08
shampoo_rate = 0.1
adam_rate = 0.02
beta_first = 0.9
beta_second = 0.95
adam_eps = 1e-08
weight_decay = 0.1
stat_decay = 0.5
second_weight = 0.3
highest = lax.Precision.HIGHEST
MESH = pl.DeviceIdType.MESH
ORDER = ("blk", "shard", "section")
VMEM_MAX = 62 * 1024 * 1024
f32 = jnp.float32
bf16 = jnp.bfloat16


def remote(src,dst,ssem,rsem,dev):
    return pltpu.make_async_remote_copy(src_ref=src,dst_ref=dst,send_sem=ssem,recv_sem=rsem,device_id=dev,device_id_type=MESH)

def split_rows(R, step, frac):
    a=int(round(R*frac/step))*step
    return min(max(a,0),R)

def ag_kernel(B,H,parts,by_section,side,counts,*refs):
    ni,no=counts
    x_ref,o_ref=refs[0],refs[1+ni]
    ssem,rsem,lsem=refs[2+ni+no:5+ni+no]
    todo=[]
    if side is not None:
        todo=side(*refs[1:1+ni],*refs[2+ni:2+ni+no],*refs[5+ni+no:])
    s=lax.axis_index("section"); b=lax.axis_index("blk"); h=lax.axis_index("shard")
    x1=h^1; y1=h^2; xy=h^3
    part=(1-s,b,h)
    xn=(s,b,x1); yn=(s,b,y1); lf=(s,b-1,h); rt=(s,b+1,h)
    has_l=b>0; has_r=b<B-1
    bar=pltpu.get_barrier_semaphore()
    for t in (part,xn,yn):
        pl.semaphore_signal(bar,inc=1,device_id=t,device_id_type=MESH)
    @pl.when(has_l)
    def _(): pl.semaphore_signal(bar,inc=1,device_id=lf,device_id_type=MESH)
    @pl.when(has_r)
    def _(): pl.semaphore_signal(bar,inc=1,device_id=rt,device_id_type=MESH)
    def slot(bb,hh,ss):
        return (ss*B+bb)*H+hh if by_section else (bb*H+hh)*2+ss
    def dst(p,bb,hh,ss): return o_ref.at[slot(bb,hh,ss),pl.ds(parts[p][0],parts[p][1])]
    def rs(p,bb,hh,ss): return rsem.at[p,slot(bb,hh,ss)]
    local=pltpu.make_async_copy(x_ref,o_ref.at[slot(b,h,s)],lsem.at[0])
    local.start()
    pl.semaphore_wait(bar,3+has_l.astype(jnp.int32)+has_r.astype(jnp.int32))
    pend=[]
    def send(p,bb,hh,ss,dev,cond=None,own=False,kind=0):
        i=len(pend)
        src=x_ref.at[pl.ds(parts[p][0],parts[p][1])] if own else dst(p,bb,hh,ss)
        cp=remote(src,dst(p,bb,hh,ss),ssem.at[i],rs(p,bb,hh,ss),dev)
        pend.append((cond,cp))
        if cond is None: cp.start()
        else:
            @pl.when(cond)
            def _(): cp.start()
    def wait(p,bb,hh,ss):
        remote(dst(p,bb,hh,ss),dst(p,bb,hh,ss),ssem.at[0],rs(p,bb,hh,ss),part).wait_recv()
    def andc(a,c):
        return c if a is None else jnp.logical_and(a,c)
    def on_arrive(cond,fn):
        if cond is None: fn()
        else: pl.when(cond)(fn)
    def group(cond,waits,sends):
        i0=len(pend)
        cps=[]
        for k,(p,bb,hh,dev,c,own) in enumerate(sends):
            src=x_ref.at[pl.ds(parts[p][0],parts[p][1])] if own else dst(p,bb,hh,s)
            cp=remote(src,dst(p,bb,hh,s),ssem.at[i0+k],rs(p,bb,hh,s),dev)
            cps.append((c,cp))
        def run():
            for (p,bb,hh) in waits: wait(p,bb,hh,s)
            for c,cp in cps:
                if c is None: cp.start()
                else: pl.when(c)(cp.start)
        on_arrive(cond,run)
        for c,cp in cps:
            cc=cond if c is None else (c if cond is None else jnp.logical_and(cond,c))
            pend.append((cc,cp))
    def work():
        if todo: todo.pop(0)()
    two=len(parts)>1
    group(None,[],[(0,b,h,rt,has_r,True),(0,b,h,lf,has_l,True),(0,b,h,xn,None,True),(0,b,h,yn,None,True)])
    if two:
        group(None,[],[(1,b,h,yn,None,True),(1,b,h,rt,has_r,True),(1,b,h,lf,has_l,True),(1,b,h,xn,None,True)])
    group(None,[],[(p,b,h,part,None,True) for p in range(len(parts))])
    if two:
        group(None,[(1,b,y1)],[(1,b,y1,rt,has_r,False),(1,b,y1,lf,has_l,False),(1,b,y1,xn,None,False),(1,b,y1,part,None,False)])
    work()
    group(None,[(0,b,x1)],[(0,b,x1,yn,None,False),(0,b,x1,part,None,False)])
    work()
    for d in range(1,B):
        cl=b>=d; cr=b+d<B
        group(cl,[(0,b-d,h)],[(0,b-d,h,rt,has_r,False),(0,b-d,h,xn,None,False),(0,b-d,h,yn,None,False),(0,b-d,h,part,None,False)])
        group(cr,[(0,b+d,h)],[(0,b+d,h,lf,has_l,False),(0,b+d,h,xn,None,False),(0,b+d,h,yn,None,False),(0,b+d,h,part,None,False)])
        if two:
            for hh in (h,y1):
                group(cl,[(1,b-d,hh)],[(1,b-d,hh,rt,has_r,False),(1,b-d,hh,xn,None,False),(1,b-d,hh,part,None,False)])
                group(cr,[(1,b+d,hh)],[(1,b+d,hh,lf,has_l,False),(1,b+d,hh,xn,None,False),(1,b+d,hh,part,None,False)])
        work()
        group(cl,[(0,b-d,x1)],[(0,b-d,x1,yn,None,False),(0,b-d,x1,part,None,False)])
        group(cr,[(0,b+d,x1)],[(0,b+d,x1,yn,None,False),(0,b+d,x1,part,None,False)])
        work()
    while todo: work()
    for d in range(B):
        for sg in ((1,-1) if d else (1,)):
            c=None if d==0 else (b+d<B if sg>0 else b>=d)
            bb=b+sg*d
            w=[(0,bb,y1),(0,bb,xy)]
            if two: w+= [(1,bb,x1),(1,bb,xy)]
            for e in w:
                group(c,[e],[(e[0],bb,e[2],part,None,False)])
    for bb in range(B):
        for hh in range(H):
            for p in range(len(parts)): wait(p,bb,hh,1-s)
    local.wait()
    for c,cp in pend:
        if c is None: cp.wait_send()
        else: pl.when(c)(cp.wait_send)

def all_gather32(x,B,H,cid,by_section=False,frac=0.636,side=None,side_in=(),side_out=(),side_scratch=()):
    R,C=x.shape
    step=16 if x.dtype==jnp.bfloat16 else 8
    a=split_rows(R,step,frac) if R>=4*step else R
    parts=[(0,a)]+([(a,R-a)] if a<R else [])
    n=2*B*H
    nsend=4+4+2+4+2+(B-1)*(8+4*4*1+4)+ (2*B-1)*4+16
    specs=[pl.BlockSpec(memory_space=pltpu.VMEM)]+[sp for _,sp in side_in]
    out=pl.pallas_call(functools.partial(ag_kernel,B,H,parts,by_section,side,(len(side_in),len(side_out))),
        out_shape=(jax.ShapeDtypeStruct((n,R,C),x.dtype),)+tuple(sh for sh,_ in side_out),
        in_specs=specs,
        out_specs=(pl.BlockSpec(memory_space=pl.ANY),)+tuple(sp for _,sp in side_out),
        scratch_shapes=[pltpu.SemaphoreType.DMA((nsend,)),pltpu.SemaphoreType.DMA((len(parts),n)),pltpu.SemaphoreType.DMA((1,))]+list(side_scratch),
        compiler_params=pltpu.CompilerParams(collective_id=cid,has_side_effects=True,vmem_limit_bytes=VMEM_MAX),name=f"gather_{R}_{cid}")(x,*[v for v,_ in side_in])
    return out if side is not None else out[0]

def rs_kernel(B,H,parts,by_section,side,counts,*refs):
    ni,no=counts
    p_ref,o_ref=refs[0],refs[1+ni]
    q,r1,ya,xa,za,xb,zb,yb,lsem,psem_s,psem_r,ssem,ya_s,xa_s,za_s,xb_s,zb_s,yb_s=refs[2+ni+no:20+ni+no]
    todo=[]
    if side is not None:
        todo=side(*refs[1:1+ni],*refs[2+ni:2+ni+no],*refs[20+ni+no:])
    def work():
        if todo: todo.pop(0)()
    s=lax.axis_index("section"); b=lax.axis_index("blk"); h=lax.axis_index("shard")
    x=h&1; y=h>>1
    part=(1-s,b,h); xn=(s,b,h^1); yn=(s,b,h^2); lf=(s,b-1,h); rt=(s,b+1,h)
    has_l=b>0; has_r=b<B-1
    bar=pltpu.get_barrier_semaphore()
    for t in (part,xn,yn):
        pl.semaphore_signal(bar,inc=1,device_id=t,device_id_type=MESH)
    @pl.when(has_l)
    def _(): pl.semaphore_signal(bar,inc=1,device_id=lf,device_id_type=MESH)
    @pl.when(has_r)
    def _(): pl.semaphore_signal(bar,inc=1,device_id=rt,device_id_type=MESH)
    (a0,an),(b0,bn)=parts
    R=an+bn
    A=pl.ds(a0,an); Bp=pl.ds(b0,bn)
    def slot(bb,hh,ss):
        return (ss*B+bb)*H+hh if by_section else (bb*H+hh)*2+ss
    low=b<B//2
    order=[]
    for i in range(B-1):
        down=B-1-i
        order.append(jnp.where(low,down-(down<=b).astype(jnp.int32),i+(i>=b).astype(jnp.int32)))
    order.append(b)
    hs=[h^3,h^2,h^1,h]
    loads={}
    for i,t in enumerate(order):
        for k in range(4):
            cp=pltpu.make_async_copy(p_ref.at[slot(t,hs[k],s)],q.at[t*H+hs[k]],lsem.at[i*4+k]); cp.start()
            loads[i,k]=cp
    pl.semaphore_wait(bar,3+has_l.astype(jnp.int32)+has_r.astype(jnp.int32))
    psend={}
    for i,t in enumerate(order):
        for k in range(4):
            cp=remote(p_ref.at[slot(t,hs[k],1-s)],r1.at[t*H+hs[k]],psem_s.at[i*4+k],psem_r.at[i*4+k],part); cp.start()
            psend[i,k]=cp
    pend=[]; late=[]
    def flush():
        while late:
            c,cp=late.pop(0)
            if c is None: cp.start()
            else: pl.when(c)(cp.start)
    def queue(c,srcr,dstr,sem,dev):
        cp=remote(srcr,dstr,ssem.at[len(pend)],sem,dev)
        pend.append((c,cp)); late.append((c,cp))
    def add(dst,a,n):
        step=next(k for k in (128,112,96,80,64,48,32,16) if n%k==0)
        @pl.loop(0,n//step)
        def _(i):
            r=pl.ds(pl.multiple_of(i*step,step),step)
            dst[r,:]=dst[r,:]+a[r,:]
    def got(dst,sem):
        remote(dst,dst,ssem.at[0],sem,part).wait_recv()
    def first(i):
        t=order[i]
        for k in range(4):
            hh=hs[k]
            loads[i,k].wait(); psend[i,k].wait_recv()
            add(q.at[t*H+hh],r1.at[t*H+hh],R)
            flush()
            if k in (0,1):
                xx=(x^1) if k==0 else x
                queue(None,q.at[t*H+hh,A],ya.at[t*2+xx],ya_s.at[t*2+xx],yn)
            if k in (0,2):
                yy=(y^1) if k==0 else y
                queue(None,q.at[t*H+hh,Bp],xb.at[t*2+yy],xb_s.at[t*2+yy],xn)
    def second(i):
        t=order[i]
        xx=x^1
        got(ya.at[t*2+xx],ya_s.at[t*2+xx])
        add(q.at[t*H+hs[2],A],ya.at[t*2+xx],an)
        flush()
        queue(None,q.at[t*H+hs[2],A],xa.at[t],xa_s.at[t],xn)
        got(xb.at[t*2+(y^1)],xb_s.at[t*2+(y^1)])
        add(q.at[t*H+hs[1],Bp],xb.at[t*2+(y^1)],bn)
        flush()
        got(ya.at[t*2+x],ya_s.at[t*2+x])
        add(q.at[t*H+h,A],ya.at[t*2+x],an)
        got(xb.at[t*2+y],xb_s.at[t*2+y])
        add(q.at[t*H+h,Bp],xb.at[t*2+y],bn)
    lines=[(hs[1],Bp,bn,lambda d,t: zb.at[(d*B+t)*2+(y^1)],lambda d,t: zb_s.at[(d*B+t)*2+(y^1)]),
           (h,Bp,bn,lambda d,t: zb.at[(d*B+t)*2+y],lambda d,t: zb_s.at[(d*B+t)*2+y]),
           (h,A,an,lambda d,t: za.at[d*B+t],lambda d,t: za_s.at[d*B+t])]
    def third(i):
        t=order[i]
        for j,(hh,rows,n,zr,zs) in enumerate(lines):
            if j==2:
                got(xa.at[t],xa_s.at[t])
                add(q.at[t*H+h,A],xa.at[t],an)
            for d,c,hin,dev in ((0,t>b,has_l,rt),(1,t<b,has_r,lf)):
                @pl.when(jnp.logical_and(c,hin))
                def _():
                    got(zr(d,t),zs(d,t))
                    add(q.at[t*H+hh,rows],zr(d,t),n)
            flush()
            for d,c,hin,dev in ((0,t>b,has_l,rt),(1,t<b,has_r,lf)):
                queue(c,q.at[t*H+hh,rows],zr(d,t),zs(d,t),dev)
    def last(j):
        hh,rows,n,zr,zs=lines[j]
        for d,hin in ((0,has_l),(1,has_r)):
            @pl.when(hin)
            def _():
                got(zr(d,b),zs(d,b))
                add(q.at[b*H+hh,rows],zr(d,b),n)
    for i in range(B+2):
        if i<B: first(i)
        work()
        if 1<=i<B+1: second(i-1)
        work()
        if 2<=i<B+1: third(i-2)
        flush()
        work()
    while todo: work()
    last(0)
    queue(None,q.at[b*H+hs[1],Bp],yb,yb_s.at[0],yn)
    got(xa.at[b],xa_s.at[b])
    add(q.at[b*H+h,A],xa.at[b],an)
    flush()
    last(1)
    last(2)
    got(yb,yb_s.at[0])
    add(q.at[b*H+h,Bp],yb,bn)
    o_ref[...]=q[b*H+h]
    for cp in psend.values(): cp.wait_send()
    for c,cp in pend:
        if c is None: cp.wait_send()
        else: pl.when(c)(cp.wait_send)

def reduce_scatter32(p,B,H,cid,by_section=False,frac=0.636,side=None,side_in=(),side_out=(),side_scratch=()):
    n,R,C=p.shape
    a=split_rows(R,16,frac)
    parts=((0,a),(a,R-a))
    V=lambda *s: pltpu.VMEM(s,p.dtype)
    D=lambda *s: pltpu.SemaphoreType.DMA(s)
    N=B*H
    an,bn=a,R-a
    nsend=4*B+B+6*(B-1)+2
    out=pl.pallas_call(functools.partial(rs_kernel,B,H,parts,by_section,side,(len(side_in),len(side_out))),
        out_shape=(jax.ShapeDtypeStruct((R,C),p.dtype),)+tuple(sh for sh,_ in side_out),
        in_specs=[pl.BlockSpec(memory_space=pl.ANY)]+[sp for _,sp in side_in],
        out_specs=(pl.BlockSpec(memory_space=pltpu.VMEM),)+tuple(sp for _,sp in side_out),
        scratch_shapes=[V(N,R,C),V(N,R,C),V(2*B,an,C),V(B,an,C),V(2*B,an,C),V(2*B,bn,C),V(4*B,bn,C),V(bn,C),
           D(N),D(N),D(N),D(nsend),D(2*B),D(B),D(2*B),D(2*B),D(4*B),D(1)]+list(side_scratch),
        compiler_params=pltpu.CompilerParams(collective_id=cid,has_side_effects=True,vmem_limit_bytes=VMEM_MAX),name=f"scatter_{R}_{cid}")(p,*[v for v,_ in side_in])
    return out if side is not None else out[0]

def swap_kernel(n,join,x_ref,o_ref,got,total,ssem,rsem,ssem2,rsem2):
    B,H=lax.axis_size("blk"),lax.axis_size("shard")
    me=(lax.axis_index("blk")*H+lax.axis_index("shard"))*2+lax.axis_index("section")
    bar=pltpu.get_barrier_semaphore()
    def place(k):
        t=(me+k)%n
        return t,(t%2,t//(2*H),(t//2)%H)
    @pl.loop(1,n)
    def _(k):
        pl.semaphore_signal(bar,inc=1,device_id=place(k)[1],device_id_type=MESH)
    pl.semaphore_wait(bar,n-1)
    if join is None:
        def copy(k):
            return remote(x_ref,o_ref.at[me],ssem.at[k],rsem.at[k],place(k)[1])
        @pl.loop(1,n)
        def _(k): copy(k).start()
        o_ref[me]=x_ref[...]
        @pl.loop(1,n)
        def _(k): copy(k).wait()
        return
    def piece(k):
        t,dev=place(k)
        return remote(x_ref.at[t],got.at[me],ssem.at[k],rsem.at[k],dev)
    def spread(k):
        return remote(total,o_ref.at[me],ssem2.at[k],rsem2.at[k],place(k)[1])
    @pl.loop(1,n)
    def _(k): piece(k).start()
    got[me]=x_ref[me]
    @pl.loop(1,n)
    def _(k): piece(k).wait()
    total[...]=join(got)
    o_ref[me]=total[...]
    @pl.loop(1,n)
    def _(k): spread(k).start()
    @pl.loop(1,n)
    def _(k): spread(k).wait()

def swap_all(x,n,cid,join=None,out_rows=None,name="swap"):
    whole=pl.BlockSpec(memory_space=pltpu.VMEM)
    D=pltpu.SemaphoreType.DMA
    C=x.shape[-1]
    R=x.shape[-2]
    out=(n,R,C) if join is None else (n,out_rows,C)
    small=(8,128) if join is None else (out_rows,C)
    return pl.pallas_call(functools.partial(swap_kernel,n,join),
        out_shape=jax.ShapeDtypeStruct(out,x.dtype),in_specs=[whole],out_specs=whole,
        scratch_shapes=[pltpu.VMEM((8,128) if join is None else (n,R,C),x.dtype),pltpu.VMEM(small,x.dtype),D((n,)),D((n,)),D((n,)),D((n,))],
        compiler_params=pltpu.CompilerParams(collective_id=cid,has_side_effects=True),name=name)(x)


def join_stats(got):
    tops=got[:,0:1,:]
    largest=jnp.max(tops,axis=0)
    return largest+jnp.log(jnp.sum(got[:,1:2,:]*jnp.exp(tops-largest),axis=0))


def join_sum(got):
    return jnp.sum(got[...],axis=0)


def gather_all(value, cid, by_section=False):
    blk, shard = lax.axis_size("blk"), lax.axis_size("shard")
    if kernels_fit():
        return all_gather32(value, blk, shard, cid, by_section)
    names = ("section", "blk", "shard") if by_section else ORDER
    return lax.all_gather(value, names)


def scatter_all(value, cid, by_section=False):
    blk, shard = lax.axis_size("blk"), lax.axis_size("shard")
    if kernels_fit():
        return reduce_scatter32(value, blk, shard, cid, by_section)
    names = ("section", "blk", "shard") if by_section else ORDER
    return lax.psum_scatter(value, names, scatter_dimension=0)


def kernels_fit():
    blk, shard = lax.axis_size("blk"), lax.axis_size("shard")
    return blk * shard <= 16 and shard == 4


def lookup_kernel(ids_ref, tab_ref, o_ref):
    rows = lax.broadcasted_iota(jnp.int32, (tab_ref.shape[0], ids_ref.shape[-1]), 0)
    hot = jnp.where(rows == ids_ref[0], 1.0, 0.0).astype(bf16)
    o_ref[0] = lax.dot_general(
        hot, tab_ref[...], (((0,), (0,)), ((), ())), preferred_element_type=f32
    ).astype(bf16)


def lookup(local_ids, table_low):
    count, tokens = local_ids.shape
    vocab = table_low.shape[0]
    return pl.pallas_call(
        lookup_kernel,
        grid=(count,),
        out_shape=jax.ShapeDtypeStruct((count, tokens, D), bf16),
        in_specs=[
            pl.BlockSpec((1, 1, tokens), lambda i: (i, 0, 0)),
            pl.BlockSpec((vocab, D), lambda i: (0, 0)),
        ],
        out_specs=pl.BlockSpec((1, tokens, D), lambda i: (i, 0, 0)),
        name="lookup",
    )(local_ids[:, None, :], table_low)


def spread_kernel(ids_ref, g_ref, base_ref, o_ref):
    rows = lax.broadcasted_iota(jnp.int32, (o_ref.shape[0], ids_ref.shape[-1]), 0)
    hot = jnp.where(rows == ids_ref[0], 1.0, 0.0).astype(bf16)

    @pl.when(pl.program_id(0) == 0)
    def _():
        o_ref[...] = base_ref[...]

    o_ref[...] += jnp.dot(hot, g_ref[0], preferred_element_type=f32)


def spread(local_ids, grads, base):
    count, tokens = local_ids.shape
    vocab = base.shape[0]
    return pl.pallas_call(
        spread_kernel,
        grid=(count,),
        out_shape=jax.ShapeDtypeStruct((vocab, D), f32),
        in_specs=[
            pl.BlockSpec((1, 1, tokens), lambda i: (i, 0, 0)),
            pl.BlockSpec((1, tokens, D), lambda i: (i, 0, 0)),
            pl.BlockSpec((vocab, D), lambda i: (0, 0)),
        ],
        out_specs=pl.BlockSpec((vocab, D), lambda i: (0, 0)),
        name="spread",
    )(local_ids[:, None, :], grads, base)


GROUP = 4


def lookup_work(ids_ref, tab_ref, o_ref, out_buf, out_sem):
    count = ids_ref.shape[0]

    def put(n):
        return pltpu.make_async_copy(out_buf.at[n % GROUP], o_ref.at[n], out_sem.at[n % GROUP])

    def step(first):
        @pl.loop(0, GROUP)
        def _(i):
            n = first + i
            if first:
                put(n - GROUP).wait()
            rows = lax.broadcasted_iota(jnp.int32, (tab_ref.shape[0], ids_ref.shape[-1]), 0)
            hot = jnp.where(rows == ids_ref[n], 1.0, 0.0).astype(bf16)
            out_buf[n % GROUP] = lax.dot_general(
                hot, tab_ref[...], (((0,), (0,)), ((), ())), preferred_element_type=f32
            ).astype(bf16)
            put(n).start()

    def finish():
        for n in range(count - GROUP, count):
            put(n).wait()

    return [functools.partial(step, n) for n in range(0, count, GROUP)] + [finish]


def gather_and_lookup(value, cid, local_ids, table_low):
    if not kernels_fit():
        return gather_all(value, cid, True), lookup(local_ids, table_low)
    count, tokens = local_ids.shape
    inside = pl.BlockSpec(memory_space=pltpu.VMEM)
    return all_gather32(
        value, lax.axis_size("blk"), lax.axis_size("shard"), cid, True,
        side=lookup_work,
        side_in=((local_ids[:, None, :], inside), (table_low, inside)),
        side_out=(
            (jax.ShapeDtypeStruct((count, tokens, D), bf16), pl.BlockSpec(memory_space=pl.ANY)),
        ),
        side_scratch=(
            pltpu.VMEM((GROUP, tokens, D), bf16),
            pltpu.SemaphoreType.DMA((GROUP,)),
        ),
    )


def spread_work(ids_ref, g_ref, base_ref, o_ref, buf, sem):
    count = ids_ref.shape[0]

    def load(first, i):
        side = (first // GROUP) % 2
        return pltpu.make_async_copy(g_ref.at[first + i], buf.at[side, i], sem.at[side, i])

    def start(first):
        for i in range(GROUP):
            load(first, i).start()

    def step(first):
        if first == 0:
            start(0)
            o_ref[...] = base_ref[...]
        if first + GROUP < count:
            start(first + GROUP)
        for i in range(GROUP):
            load(first, i).wait()

        @pl.loop(0, GROUP)
        def _(i):
            rows = lax.broadcasted_iota(jnp.int32, (o_ref.shape[0], ids_ref.shape[-1]), 0)
            hot = jnp.where(rows == ids_ref[first + i], 1.0, 0.0).astype(bf16)
            o_ref[...] += jnp.dot(
                hot, buf[(first // GROUP) % 2, i], preferred_element_type=f32
            )

    return [functools.partial(step, n) for n in range(0, count, GROUP)]


def scatter_and_spread(value, cid, local_ids, grads, base):
    if not kernels_fit():
        return scatter_all(value, cid, True), spread(local_ids, grads, base)
    tokens = local_ids.shape[1]
    inside = pl.BlockSpec(memory_space=pltpu.VMEM)
    return reduce_scatter32(
        value, lax.axis_size("blk"), lax.axis_size("shard"), cid, True,
        side=spread_work,
        side_in=(
            (local_ids[:, None, :], inside),
            (grads, pl.BlockSpec(memory_space=pl.ANY)),
            (base, inside),
        ),
        side_out=((jax.ShapeDtypeStruct(base.shape, f32), inside),),
        side_scratch=(
            pltpu.VMEM((2, GROUP, tokens, D), bf16),
            pltpu.SemaphoreType.DMA((2, GROUP)),
        ),
    )


def stats_kernel(vocab, nf_ref, tab_ref, t0_ref, t1_ref, top_ref, sum_ref, exp_ref, pick_ref):
    logits = lax.dot_general(
        tab_ref[...], nf_ref[0], (((1,), (1,)), ((), ())), preferred_element_type=f32
    )
    rows = lax.broadcasted_iota(jnp.int32, logits.shape, 0)
    hits = jnp.where(rows == t0_ref[0], 1.0, 0.0) + jnp.where(rows == t1_ref[0], second_weight, 0.0)

    @pl.when(pl.program_id(0) == 0)
    def _():
        pick_ref[...] = jnp.zeros_like(pick_ref)

    pick_ref[...] += jnp.sum(hits * logits, axis=0, keepdims=True)
    logits = jnp.where(rows < vocab, logits, -1e30)
    top = jnp.max(logits, axis=0, keepdims=True)
    expo = jnp.exp(logits - top)
    top_ref[0] = top
    sum_ref[0] = jnp.sum(expo, axis=0, keepdims=True)
    exp_ref[0] = expo.astype(bf16)


def vocab_stats(normed, table_low, first, second, vocab):
    count, tokens, _ = normed.shape
    padded = table_low.shape[0]
    row = jax.ShapeDtypeStruct((count, 1, tokens), f32)
    row_spec = pl.BlockSpec((1, 1, tokens), lambda i: (i, 0, 0))
    return pl.pallas_call(
        functools.partial(stats_kernel, vocab),
        grid=(count,),
        out_shape=(
            row, row, jax.ShapeDtypeStruct((count, padded, tokens), bf16),
            jax.ShapeDtypeStruct((1, tokens), f32),
        ),
        in_specs=[
            pl.BlockSpec((1, tokens, D), lambda i: (i, 0, 0)),
            pl.BlockSpec((padded, D), lambda i: (0, 0)),
            row_spec,
            row_spec,
        ],
        out_specs=(
            row_spec,
            row_spec,
            pl.BlockSpec((1, padded, tokens), lambda i: (i, 0, 0)),
            pl.BlockSpec((1, tokens), lambda i: (0, 0)),
        ),
        name="vocab_stats",
    )(normed, table_low, first[:, None, :], second[:, None, :])


def vocab_kernel(scale, exp_ref, nf_ref, tab_ref, top_ref, lse_ref, t0_ref, t1_ref, g_ref, acc_ref):
    rows = lax.broadcasted_iota(jnp.int32, exp_ref.shape[1:], 0)
    hits = jnp.where(rows == t0_ref[0], scale, 0.0) + jnp.where(
        rows == t1_ref[0], second_weight * scale, 0.0
    )
    weight = jnp.exp(top_ref[0] - lse_ref[0]) * ((1.0 + second_weight) * scale)
    grad = (exp_ref[0].astype(f32) * weight - hits).astype(bf16)

    @pl.when(pl.program_id(0) == 0)
    def _():
        acc_ref[...] = jnp.zeros_like(acc_ref)

    g_ref[0] = lax.dot_general(
        grad, tab_ref[...], (((0,), (0,)), ((), ())), preferred_element_type=f32
    ).astype(bf16)
    acc_ref[...] += jnp.dot(grad, nf_ref[0], preferred_element_type=f32)


def vocab_grads(expo, normed, table_low, top, log_total, first, second, scale):
    count, tokens, _ = normed.shape
    padded = table_low.shape[0]
    row = pl.BlockSpec((1, 1, tokens), lambda i: (i, 0, 0))
    return pl.pallas_call(
        functools.partial(vocab_kernel, scale),
        grid=(count,),
        out_shape=(
            jax.ShapeDtypeStruct((count, tokens, D), bf16),
            jax.ShapeDtypeStruct((padded, D), f32),
        ),
        in_specs=[
            pl.BlockSpec((1, padded, tokens), lambda i: (i, 0, 0)),
            pl.BlockSpec((1, tokens, D), lambda i: (i, 0, 0)),
            pl.BlockSpec((padded, D), lambda i: (0, 0)),
            row,
            row,
            row,
            row,
        ],
        out_specs=(
            pl.BlockSpec((1, tokens, D), lambda i: (i, 0, 0)),
            pl.BlockSpec((padded, D), lambda i: (0, 0)),
        ),
        name="vocab_grads",
    )(expo, normed, table_low, top, log_total[:, None, :], first[:, None, :], second[:, None, :])


CORNER = (0, 3, 1, 2)


def place_of(index, shard):
    turn, group = index % 4, index // 4
    side = ((turn + 1) // 2) % 2
    return (turn // 2, group // (shard // 2), 2 * (group % (shard // 2)) + side)


def my_block():
    shard = lax.axis_size("shard")
    section, h = lax.axis_index("section"), lax.axis_index("shard")
    side = h % 2
    return (lax.axis_index("blk") * (shard // 2) + h // 2) * 4 + side + section * (3 - 2 * side)


def meet(reach, block, blocks, mine, shard, sign):
    barrier = pltpu.get_barrier_semaphore()
    above = [block + d < blocks for d in range(1, reach + 1)]
    below = [block >= d for d in range(1, reach + 1)]
    sources, targets = (below, above) if sign > 0 else (above, below)
    for d in range(1, reach + 1):

        @pl.when(sources[d - 1])
        def _():
            pl.semaphore_signal(
                barrier, inc=1, device_id=place_of(mine - sign * d, shard), device_id_type=MESH
            )

    @pl.when(targets[0])
    def _():
        pl.semaphore_wait(barrier, sum(held.astype(jnp.int32) for held in targets))


def half_masks(tokens):
    lane = lax.broadcasted_iota(jnp.int32, (tokens, 2 * HEAD_DIM), 1)
    return lane < HEAD_DIM


def allowed_mask(d, seg_ref, tokens):
    own = jnp.transpose(jnp.broadcast_to(seg_ref[0], (128, tokens)))[:, :1]
    allowed = own == seg_ref[d]
    if d == 0:
        row = lax.broadcasted_iota(jnp.int32, (tokens, tokens), 0)
        col = lax.broadcasted_iota(jnp.int32, (tokens, tokens), 1)
        allowed = allowed & (col <= row)
    return allowed


def attend_kernel(reach, blocks, q_ref, k_ref, v_ref, seg_ref, tot_ref, acc_ref, kr_ref, vr_ref,
                  send_sem, recv_sem):
    shard = lax.axis_size("shard")
    mine = my_block()
    block = mine % blocks
    tokens = q_ref.shape[0]
    meet(reach, block, blocks, mine, shard, 1)

    def copies(d):
        target = place_of(mine + d, shard)
        return [
            pltpu.make_async_remote_copy(
                src_ref=source,
                dst_ref=target_ref.at[d - 1],
                send_sem=send_sem.at[d - 1, i],
                recv_sem=recv_sem.at[d - 1, i],
                device_id=target,
                device_id_type=MESH,
            )
            for i, (source, target_ref) in enumerate(((k_ref, kr_ref), (v_ref, vr_ref)))
        ]

    for d in range(reach, 0, -1):

        @pl.when(block + d < blocks)
        def _():
            for copy in copies(d):
                copy.start()

    scale = HEAD_DIM ** (-0.5)
    left = half_masks(tokens)
    zero = jnp.zeros((tokens, 2 * HEAD_DIM), bf16)

    def visit(d, keys, values):
        allowed = allowed_mask(d, seg_ref, tokens)

        @pl.loop(0, HEADS // 2)
        def _(pair):
            lanes = pl.ds(pl.multiple_of(pair * 128, 128), 128)
            q_pair, k_pair, v_pair = q_ref[:, lanes], keys[:, lanes], values[:, lanes]
            totals, sums = [], []
            for side in (left, ~left):
                scores = lax.dot_general(
                    jnp.where(side, q_pair, zero),
                    k_pair,
                    (((1,), (1,)), ((), ())),
                    preferred_element_type=f32,
                )
                expo = jnp.where(allowed, jnp.exp(scores * scale), 0.0)
                totals.append(jnp.sum(expo, axis=1, keepdims=True))
                sums.append(jnp.dot(expo.astype(bf16), v_pair, preferred_element_type=f32))
            total = jnp.where(left, totals[0], totals[1])
            added = jnp.where(left, sums[0], sums[1])
            if d == 0:
                tot_ref[:, lanes] = total
                acc_ref[:, lanes] = added
            else:
                tot_ref[:, lanes] += total
                acc_ref[:, lanes] += added

    visit(0, k_ref, v_ref)
    for d in range(1, reach + 1):

        @pl.when(block >= d)
        def _():
            for copy in copies(d):
                copy.wait_recv()
            visit(d, kr_ref.at[d - 1], vr_ref.at[d - 1])

    for d in range(1, reach + 1):

        @pl.when(block + d < blocks)
        def _():
            for copy in copies(d):
                copy.wait_send()


def attend(q, k, v, seg_rows, reach, blocks, cid):
    tokens = q.shape[0]
    wide = jax.ShapeDtypeStruct((tokens, D), f32)
    far = jax.ShapeDtypeStruct((reach, tokens, D), bf16)
    whole = pl.BlockSpec(memory_space=pltpu.VMEM)
    return pl.pallas_call(
        functools.partial(attend_kernel, reach, blocks),
        out_shape=(wide, wide, far, far),
        in_specs=[whole] * 4,
        out_specs=(whole,) * 4,
        scratch_shapes=[
            pltpu.SemaphoreType.DMA((reach, 2)),
            pltpu.SemaphoreType.DMA((reach, 2)),
        ],
        compiler_params=pltpu.CompilerParams(
            collective_id=cid, has_side_effects=True, vmem_limit_bytes=VMEM_MAX
        ),
        name="attend",
    )(q, k, v, seg_rows)


def attend_back_kernel(reach, blocks, q_ref, k_ref, v_ref, kr_ref, vr_ref, tot_ref, acc_ref, ga_ref,
                       seg_ref, dq_ref, dk_ref, dv_ref, gw, gt, far_k, far_v, got_k, got_v,
                       send_sem, recv_sem):
    shard = lax.axis_size("shard")
    mine = my_block()
    block = mine % blocks
    tokens = q_ref.shape[0]
    meet(reach, block, blocks, mine, shard, -1)
    scale = HEAD_DIM ** (-0.5)
    left = half_masks(tokens)
    zero = jnp.zeros((tokens, 2 * HEAD_DIM), bf16)

    @pl.loop(0, HEADS // 2)
    def _(pair):
        lanes = pl.ds(pl.multiple_of(pair * 128, 128), 128)
        inverse = 1.0 / tot_ref[:, lanes]
        grad = ga_ref[:, lanes]
        gw[:, lanes] = (grad * inverse).astype(bf16)
        product = grad * acc_ref[:, lanes]
        first = jnp.sum(jnp.where(left, product, 0.0), axis=1, keepdims=True)
        second = jnp.sum(jnp.where(left, 0.0, product), axis=1, keepdims=True)
        gt[:, lanes] = -jnp.where(left, first, second) * inverse * inverse
        dq_ref[:, lanes] = jnp.zeros((tokens, 128), f32)

    def visit(d, keys, values, out_k, out_v):
        allowed = allowed_mask(d, seg_ref, tokens)

        @pl.loop(0, HEADS // 2)
        def _(pair):
            lanes = pl.ds(pl.multiple_of(pair * 128, 128), 128)
            q_pair, k_pair, v_pair, w_pair = q_ref[:, lanes], keys[:, lanes], values[:, lanes], gw[:, lanes]
            gt_pair = gt[:, lanes]
            dq, dk, dv = [], [], []
            for i, side in enumerate((left, ~left)):
                scores = lax.dot_general(
                    jnp.where(side, q_pair, zero),
                    k_pair,
                    (((1,), (1,)), ((), ())),
                    preferred_element_type=f32,
                )
                expo = jnp.where(allowed, jnp.exp(scores * scale), 0.0)
                probs = lax.dot_general(
                    jnp.where(side, w_pair, zero),
                    v_pair,
                    (((1,), (1,)), ((), ())),
                    preferred_element_type=f32,
                )
                part = (expo * (probs + gt_pair[:, i * HEAD_DIM : i * HEAD_DIM + 1])).astype(bf16)
                dq.append(jnp.dot(part, k_pair, preferred_element_type=f32))
                dk.append(
                    lax.dot_general(part, q_pair, (((0,), (0,)), ((), ())), preferred_element_type=f32)
                )
                dv.append(
                    lax.dot_general(
                        expo.astype(bf16), w_pair, (((0,), (0,)), ((), ())), preferred_element_type=f32
                    )
                )
            dq_ref[:, lanes] += jnp.where(left, dq[0], dq[1]) * scale
            out_k[:, lanes] = (jnp.where(left, dk[0], dk[1]) * scale).astype(out_k.dtype)
            out_v[:, lanes] = jnp.where(left, dv[0], dv[1]).astype(out_v.dtype)

    def copies(d):
        target = place_of(mine - d, shard)
        return [
            pltpu.make_async_remote_copy(
                src_ref=source.at[d - 1],
                dst_ref=target_ref.at[d - 1],
                send_sem=send_sem.at[d - 1, i],
                recv_sem=recv_sem.at[d - 1, i],
                device_id=target,
                device_id_type=MESH,
            )
            for i, (source, target_ref) in enumerate(((far_k, got_k), (far_v, got_v)))
        ]

    for d in range(reach, 0, -1):

        @pl.when(block >= d)
        def _():
            visit(d, kr_ref.at[d - 1], vr_ref.at[d - 1], far_k.at[d - 1], far_v.at[d - 1])
            for copy in copies(d):
                copy.start()

    visit(0, k_ref, v_ref, dk_ref, dv_ref)
    for d in range(reach, 0, -1):

        @pl.when(block + d < blocks)
        def _():
            for copy in copies(d):
                copy.wait_recv()
            dk_ref[...] += got_k[d - 1].astype(f32)
            dv_ref[...] += got_v[d - 1].astype(f32)

    for d in range(1, reach + 1):

        @pl.when(block >= d)
        def _():
            for copy in copies(d):
                copy.wait_send()


def attend_back(q, k, v, far_k, far_v, total, accum, grad, seg_rows, reach, blocks, cid):
    tokens = q.shape[0]
    wide = jax.ShapeDtypeStruct((tokens, D), f32)
    whole = pl.BlockSpec(memory_space=pltpu.VMEM)
    return pl.pallas_call(
        functools.partial(attend_back_kernel, reach, blocks),
        out_shape=(wide, wide, wide),
        in_specs=[whole] * 9,
        out_specs=(whole,) * 3,
        scratch_shapes=[pltpu.VMEM((tokens, D), bf16), pltpu.VMEM((tokens, D), f32)]
        + [pltpu.VMEM((reach, tokens, D), bf16)] * 4
        + [pltpu.SemaphoreType.DMA((reach, 2)), pltpu.SemaphoreType.DMA((reach, 2))],
        compiler_params=pltpu.CompilerParams(
            collective_id=cid, has_side_effects=True, vmem_limit_bytes=VMEM_MAX
        ),
        name="attend_back",
    )(q, k, v, far_k, far_v, total, accum, grad, seg_rows)


def matrix_layout():
    return ((D, 3 * D), (D, D), (D, 2 * FF), (FF, D))


def blocks_to_rows(blocks):
    count = blocks.shape[0]
    if count % 4:
        return blocks.reshape(-1, QUAD)
    quads = blocks.reshape(count // 4, 4, BS, BS).transpose(0, 2, 1, 3)
    return quads.reshape(-1, QUAD)


def rows_to_blocks(rows):
    count = rows.shape[0] * QUAD // (BS * BS)
    if count % 4:
        return rows.reshape(count, BS, BS)
    return rows.reshape(count // 4, BS, 4, BS).transpose(0, 2, 1, 3).reshape(count, BS, BS)


def rows_to_quads(rows, count):
    if count % 4:
        rows = rows.reshape(-1, 4, BS, BS).transpose(0, 2, 1, 3)
    return rows.reshape(-1, BS, QUAD)


def quads_to_rows(quads, count):
    if count % 4:
        quads = quads.reshape(-1, BS, 4, BS).transpose(0, 2, 1, 3)
    return quads.reshape(-1, count * BS * BS // QUAD, QUAD)


def rope_tables(positions):
    half_dim = HEAD_DIM // 2
    frequency = rope_base ** (-jnp.arange(half_dim, dtype=f32) * 2.0 / HEAD_DIM)
    angles = positions.astype(f32)[:, None] * frequency[None, :]
    cosine, sine = jnp.cos(angles), jnp.sin(angles)
    return (
        jnp.concatenate([cosine, cosine] * 4, axis=-1),
        jnp.concatenate([-sine, sine] * 4, axis=-1),
    )


QKV, OUT, GATE, DOWN = (0, 12, 9), (108, 12, 3), (144, 12, 16), (336, 32, 3)
QUADS = 432
WHOLE = pl.BlockSpec(memory_space=pltpu.VMEM)
LEFT = pl.BlockSpec(memory_space=pl.ANY)


def struct(shape, dtype=f32):
    return jax.ShapeDtypeStruct(shape, dtype)


def column(buf, kind, c, base=0):
    offset, rows, cols = kind
    return jnp.concatenate([buf[offset - base + r * cols + c] for r in range(rows)], axis=0)


def band(buf, kind, r, base=0):
    offset, _, cols = kind
    return jnp.concatenate(
        [
            jnp.concatenate([buf[offset - base + (4 * r + i) * cols + c] for c in range(cols)], axis=1)
            for i in range(4)
        ],
        axis=0,
    )


def lanes_of(c):
    return pl.ds(pl.multiple_of(c * QUAD, QUAD), QUAD)


def dot(left_side, right_side):
    return jnp.dot(left_side, right_side, preferred_element_type=f32)


def dot_nt(left_side, right_side):
    return lax.dot_general(
        left_side, right_side, (((1,), (1,)), ((), ())), preferred_element_type=f32
    )


def norm_of(x):
    return lax.rsqrt(jnp.mean(x * x, axis=-1, keepdims=True) + norm_eps)


def norm_back(x, gain, grad):
    inverse = norm_of(x)
    weighted = grad * gain
    grad_in = inverse * weighted - x * (inverse * inverse * inverse) * jnp.mean(
        weighted * x, axis=-1, keepdims=True
    )
    return grad_in, jnp.sum(grad * x * inverse, axis=0, keepdims=True)


def swapped(u):
    lane = lax.broadcasted_iota(jnp.int32, u.shape, 1)
    half = HEAD_DIM // 2
    return jnp.where(
        lane % HEAD_DIM < half, pltpu.roll(u, u.shape[1] - half, 1), pltpu.roll(u, half, 1)
    )


def load_quads(w_ref, layer, kinds, bufs, sem):
    copies = []
    for i, ((offset, rows, cols), buf) in enumerate(zip(kinds, bufs)):
        copy = pltpu.make_async_copy(w_ref.at[layer, pl.ds(offset, rows * cols)], buf, sem.at[i])
        copy.start()
        copies.append(copy)
    return copies


def quad_buffers(kinds):
    return [pltpu.VMEM((rows * cols, BS, QUAD), bf16) for _, rows, cols in kinds] + [
        pltpu.SemaphoreType.DMA((len(kinds),))
    ]


def big(**extra):
    return pltpu.CompilerParams(vmem_limit_bytes=VMEM_MAX, **extra)


def qkv_kernel(layer, x_ref, gain_ref, cos_ref, sin_ref, w_ref, a_ref, q_ref, k_ref, v_ref, wq, sem):
    (copy,) = load_quads(w_ref, layer, (QKV,), (wq,), sem)
    x = x_ref[...]
    a_ref[...] = (x * norm_of(x) * gain_ref[...]).astype(bf16)
    copy.wait()
    for i, out in enumerate((q_ref, k_ref, v_ref)):

        @pl.loop(0, 3)
        def _(c):
            part = dot(a_ref[...], column(wq, QKV, 3 * i + c, QKV[0]))
            if i < 2:
                part = part * cos_ref[...] + swapped(part) * sin_ref[...]
            out[:, lanes_of(c)] = part.astype(bf16)


def qkv_forward(layer, x, gain, cosine, sine, quads):
    tokens = x.shape[0]
    low = struct((tokens, D), bf16)
    return pl.pallas_call(
        functools.partial(qkv_kernel, layer),
        out_shape=(low,) * 4,
        in_specs=[WHOLE] * 4 + [LEFT],
        out_specs=(WHOLE,) * 4,
        scratch_shapes=quad_buffers((QKV,)),
        compiler_params=big(),
        name="qkv",
    )(x, gain, cosine, sine, quads)


def mlp_kernel(layer, last, x_ref, acc_ref, tot_ref, gain_ref, final_ref, w_ref, out_ref, att_ref,
               mixed_ref, nm_ref, gate_ref, up_ref, hid_ref, nf_ref, wo, wg, wd, sem):
    copies = load_quads(w_ref, layer, (OUT, GATE, DOWN), (wo, wg, wd), sem)
    att_ref[...] = (acc_ref[...] / tot_ref[...]).astype(bf16)
    copies[0].wait()

    @pl.loop(0, 3)
    def _(c):
        lanes = lanes_of(c)
        mixed_ref[:, lanes] = x_ref[:, lanes] + dot(att_ref[...], column(wo, OUT, c, OUT[0]))

    mixed = mixed_ref[...]
    nm_ref[...] = (mixed * norm_of(mixed) * gain_ref[...]).astype(bf16)
    copies[1].wait()

    @pl.loop(0, FF // QUAD)
    def _(c):
        lanes = lanes_of(c)
        gate = dot(nm_ref[...], column(wg, GATE, c, GATE[0]))
        upper = dot(nm_ref[...], column(wg, GATE, c + FF // QUAD, GATE[0]))
        gate_ref[:, lanes] = gate
        up_ref[:, lanes] = upper
        hid_ref[:, lanes] = (gate / (1.0 + jnp.exp(-gate)) * upper).astype(bf16)

    copies[2].wait()

    @pl.loop(0, 3)
    def _(c):
        lanes = lanes_of(c)
        out_ref[:, lanes] = mixed_ref[:, lanes] + dot(hid_ref[...], column(wd, DOWN, c, DOWN[0]))

    if last:
        out = out_ref[...]
        nf_ref[...] = (out * norm_of(out) * final_ref[...]).astype(bf16)
    else:
        nf_ref[...] = jnp.zeros_like(nf_ref)


def mlp_forward(layer, last, x, accum, total, gain, final_gain, quads):
    tokens = x.shape[0]
    wide, low = struct((tokens, D)), struct((tokens, D), bf16)
    return pl.pallas_call(
        functools.partial(mlp_kernel, layer, last),
        out_shape=(
            wide, low, wide, low, struct((tokens, FF)), struct((tokens, FF)),
            struct((tokens, FF), bf16), low,
        ),
        in_specs=[WHOLE] * 5 + [LEFT],
        out_specs=(WHOLE,) * 8,
        scratch_shapes=quad_buffers((OUT, GATE, DOWN)),
        compiler_params=big(),
        name="mlp",
    )(x, accum, total, gain, final_gain, quads)


def put_quads(buf, kind, c, value, base):
    offset, rows, cols = kind
    for r in range(rows):
        buf[offset - base + r * cols + c] = value[r * BS : (r + 1) * BS].astype(bf16)


def mlp_back_kernel(layer, last, first_call, *refs):
    (gy_ref, h_ref, mixed_ref, nm_ref, gate_ref, up_ref, hid_ref, att_ref, gain_ref, final_ref,
     w_ref) = refs[:11]
    (p_ref, gm_ref, gatt_ref, gg_ref, gf_ref, wo, wg, wd, sem, grads, gl, ggu, turned, gin,
     out_sem) = refs[11 + (not first_call):]
    copies = load_quads(w_ref, layer, (DOWN, GATE, OUT), (wd, wg, wo), sem)
    base = OUT[0]
    if last:
        grad, gain_row = norm_back(h_ref[...], final_ref[...], gy_ref[...].astype(f32))
        gf_ref[...] = gain_row
    else:
        grad = gy_ref[...]
        gf_ref[...] = jnp.zeros_like(gf_ref)
    gin[...] = grad
    gl[...] = grad.astype(bf16)
    copies[0].wait()

    @pl.loop(0, FF // QUAD)
    def _(r):
        lanes = lanes_of(r)
        grad_down = dot(jnp.transpose(hid_ref[:, lanes]), gl[...])
        for i in range(4):
            for c in range(3):
                grads[DOWN[0] - base + (4 * r + i) * 3 + c] = grad_down[
                    i * BS : (i + 1) * BS, c * QUAD : (c + 1) * QUAD
                ].astype(bf16)
        grad_hidden = dot_nt(gl[...], band(wd, DOWN, r, DOWN[0]))
        gate, upper = gate_ref[:, lanes], up_ref[:, lanes]
        sig = 1.0 / (1.0 + jnp.exp(-gate))
        ggu[:, lanes] = (grad_hidden * upper * sig * (1.0 + gate * (1.0 - sig))).astype(bf16)
        ggu[:, lanes_of(r + FF // QUAD)] = (grad_hidden * gate * sig).astype(bf16)

    def send(i, kind):
        offset, rows, cols = kind
        copy = pltpu.make_async_copy(
            grads.at[pl.ds(offset - base, rows * cols)],
            p_ref.at[layer, pl.ds(offset, rows * cols)],
            out_sem.at[i],
        )
        copy.start()
        return copy

    sent = [send(0, DOWN)]
    turned[...] = jnp.transpose(nm_ref[...])
    gatt_ref[...] = jnp.zeros_like(gatt_ref)
    copies[1].wait()

    @pl.loop(0, 2 * FF // QUAD)
    def _(c):
        part = ggu[:, lanes_of(c)]
        put_quads(grads, GATE, c, dot(turned[...], part), base)
        gatt_ref[...] += dot_nt(part, column(wg, GATE, c, GATE[0]))

    sent.append(send(1, GATE))
    grad_norm, gain_row = norm_back(mixed_ref[...], gain_ref[...], gatt_ref[...])
    gg_ref[...] = gain_row
    grad_mixed = gin[...] + grad_norm
    gm_ref[...] = grad_mixed
    gl[...] = grad_mixed.astype(bf16)
    turned[...] = jnp.transpose(att_ref[...])
    gatt_ref[...] = jnp.zeros_like(gatt_ref)
    copies[2].wait()

    @pl.loop(0, 3)
    def _(c):
        part = gl[:, lanes_of(c)]
        put_quads(grads, OUT, c, dot(turned[...], part), base)
        gatt_ref[...] += dot_nt(part, column(wo, OUT, c, OUT[0]))

    sent.append(send(2, OUT))
    for copy in sent:
        copy.wait()


def mlp_backward(layer, last, grad, states, cache, gain, final_gain, quads, store):
    mixed, nm, gate, upper, hidden, att = cache
    tokens = mixed.shape[0]
    wide, row = struct((tokens, D)), struct((1, D))
    kinds = (DOWN, GATE, OUT)
    buffers = quad_buffers((OUT, GATE, DOWN))
    operands = [grad, states, mixed, nm, gate, upper, hidden, att, gain, final_gain, quads]
    aliases = {}
    if store is not None:
        operands.append(store)
        aliases = {11: 0}
    return pl.pallas_call(
        functools.partial(mlp_back_kernel, layer, last, store is None),
        out_shape=(struct((2, QUADS, BS, QUAD), bf16), wide, wide, row, row),
        in_specs=[WHOLE] * 10 + [LEFT] * (len(operands) - 10),
        out_specs=(LEFT,) + (WHOLE,) * 4,
        scratch_shapes=buffers
        + [
            pltpu.VMEM((QUADS - OUT[0], BS, QUAD), bf16),
            pltpu.VMEM((tokens, D), bf16),
            pltpu.VMEM((tokens, 2 * FF), bf16),
            pltpu.VMEM((D, tokens), bf16),
            pltpu.VMEM((tokens, D), f32),
            pltpu.SemaphoreType.DMA((3,)),
        ],
        input_output_aliases=aliases,
        compiler_params=big(),
        name="mlp_back",
    )(*operands)


def qkv_back_kernel(layer, dq_ref, dk_ref, dv_ref, a_ref, x_ref, gm_ref, gain_ref, cos_ref, sin_ref,
                    w_ref, store_ref, p_ref, gx_ref, low_ref, gg_ref, wq, sem, grads, turned, out_sem):
    (copy,) = load_quads(w_ref, layer, (QKV,), (wq,), sem)
    turned[...] = jnp.transpose(a_ref[...])
    gx_ref[...] = jnp.zeros_like(gx_ref)
    copy.wait()
    for i, ref in enumerate((dq_ref, dk_ref, dv_ref)):

        @pl.loop(0, 3)
        def _(c):
            part = ref[:, lanes_of(c)]
            if i < 2:
                part = part * cos_ref[...] - swapped(part) * sin_ref[...]
            part = part.astype(bf16)
            put_quads(grads, QKV, 3 * i + c, dot(turned[...], part), QKV[0])
            gx_ref[...] += dot_nt(part, column(wq, QKV, 3 * i + c, QKV[0]))

    out = pltpu.make_async_copy(
        grads, p_ref.at[layer, pl.ds(QKV[0], QKV[1] * QKV[2])], out_sem.at[0]
    )
    out.start()
    grad_norm, gain_row = norm_back(x_ref[...], gain_ref[...], gx_ref[...])
    gg_ref[...] = gain_row
    grad = gm_ref[...] + grad_norm
    gx_ref[...] = grad
    low_ref[...] = grad.astype(bf16)
    out.wait()


def qkv_backward(layer, dq, dk, dv, a, x, grad_mixed, gain, cosine, sine, quads, store):
    tokens = x.shape[0]
    return pl.pallas_call(
        functools.partial(qkv_back_kernel, layer),
        out_shape=(
            struct((2, QUADS, BS, QUAD), bf16), struct((tokens, D)), struct((tokens, D), bf16),
            struct((1, D)),
        ),
        in_specs=[WHOLE] * 9 + [LEFT] * 2,
        out_specs=(LEFT,) + (WHOLE,) * 3,
        scratch_shapes=quad_buffers((QKV,))
        + [
            pltpu.VMEM((QKV[1] * QKV[2], BS, QUAD), bf16),
            pltpu.VMEM((D, tokens), bf16),
            pltpu.SemaphoreType.DMA((1,)),
        ],
        input_output_aliases={10: 0},
        compiler_params=big(),
        name="qkv_back",
    )(dq, dk, dv, a, x, grad_mixed, gain, cosine, sine, quads, store)


def shampoo_kernel(scale_ref, g_ref, w_ref, ls_ref, rs_ref, lr_ref, rr_ref, wn_ref, wl_ref, ln_ref,
                   rn_ref):
    factor = scale_ref[0, 0]
    row = lax.broadcasted_iota(jnp.int32, (QUAD, QUAD), 0)
    col = lax.broadcasted_iota(jnp.int32, (QUAD, QUAD), 1)
    same = (row // BS) == (col // BS)

    def diagonal(wide):
        return jnp.where(same, jnp.concatenate([wide] * 4, axis=0), jnp.zeros((), wide.dtype))

    for j in range(g_ref.shape[0]):

        def side(ref):
            return jnp.concatenate([ref[4 * j + i] for i in range(4)], axis=1).astype(bf16)

        g = g_ref[j]
        left = dot_nt(g, diagonal(g)) * (factor * factor * (1.0 - stat_decay))
        right = lax.dot_general(g, g, (((0,), (0,)), ((), ())), preferred_element_type=f32)
        right = right * (factor * factor * (1.0 - stat_decay))
        inner = dot(g, diagonal(side(rr_ref))) * factor
        step = dot(side(lr_ref), diagonal(inner.astype(bf16)))
        for i in range(4):
            cut = slice(i * BS, (i + 1) * BS)
            n = 4 * j + i
            ln_ref[n] = stat_decay * ls_ref[n] + left[:, cut]
            rn_ref[n] = stat_decay * rs_ref[n] + right[cut, cut]
            new = w_ref[n] - shampoo_rate * step[:, cut]
            wn_ref[n] = new
            wl_ref[n] = new.astype(bf16)


def shampoo(factor, rows, weights, left_stats, right_stats, left_root, right_root):
    count = weights.shape[0]
    quads = 3
    square = pl.BlockSpec((4 * quads, BS, BS), lambda i: (i, 0, 0))
    return pl.pallas_call(
        shampoo_kernel,
        grid=(count // (4 * quads),),
        out_shape=(
            struct((count, BS, BS)), struct((count, BS, BS), bf16), struct((count, BS, BS)),
            struct((count, BS, BS)),
        ),
        in_specs=[
            pl.BlockSpec(memory_space=pltpu.SMEM),
            pl.BlockSpec((quads, BS, QUAD), lambda i: (i, 0, 0)),
        ]
        + [square] * 5,
        out_specs=(square,) * 4,
        name="shampoo",
    )(
        factor.reshape(1, 1), rows.reshape(-1, BS, QUAD), weights, left_stats, right_stats,
        left_root, right_root,
    )


def shampoo_plain(factor, rows, weights, left_stats, right_stats, left_root, right_root):
    grads = rows_to_blocks(rows.astype(f32)) * factor
    left_new = stat_decay * left_stats + (1.0 - stat_decay) * jnp.einsum(
        "bij,bkj->bik", grads, grads, precision=highest
    )
    right_new = stat_decay * right_stats + (1.0 - stat_decay) * jnp.einsum(
        "bji,bjk->bik", grads, grads, precision=highest
    )
    direction = jnp.einsum(
        "bij,bjk->bik",
        left_root,
        jnp.einsum("bij,bjk->bik", grads, right_root, precision=highest),
        precision=highest,
    )
    new = weights - shampoo_rate * direction
    return new, new.astype(bf16), left_new, right_new


def adam_step(weight, first, second, grad_in, decay):
    first_new = beta_first * first + (1.0 - beta_first) * grad_in
    second_new = beta_second * second + (1.0 - beta_second) * grad_in * grad_in
    weight_new = weight - adam_rate * (
        first_new / (jnp.sqrt(second_new) + adam_eps) + decay * weight
    )
    return (weight_new, first_new, second_new)


def share_ids(packed, cid):
    blk, shard = lax.axis_size("blk"), lax.axis_size("shard")
    if kernels_fit():
        every = swap_all(packed, 2 * blk * shard, cid, name="swap_ids")
        return every.reshape(blk, shard, 2, *packed.shape)[:, :, 0]
    return lax.all_gather(packed, ("blk", "shard")).reshape(blk, shard, *packed.shape)


def share_stats(top, total, cid):
    blk, shard = lax.axis_size("blk"), lax.axis_size("shard")
    devices = 2 * blk * shard
    if kernels_fit():
        pair = jnp.concatenate([top, total], axis=1)
        return swap_all(pair, devices, cid, join_stats, 1, name="swap_stats")[:, 0]
    largest = lax.pmax(top[:, 0], ORDER)
    return largest + jnp.log(lax.psum(total[:, 0] * jnp.exp(top[:, 0] - largest), ORDER))


def share_sum(small, cid):
    blk, shard = lax.axis_size("blk"), lax.axis_size("shard")
    devices = 2 * blk * shard
    if kernels_fit():
        lanes = pl.cdiv(small.size, devices * 128) * 128
        flat = jnp.pad(small.reshape(-1), (0, devices * lanes - small.size))
        every = swap_all(flat.reshape(devices, 1, lanes), devices, cid, join_sum, 1, name="swap_sum")
        return every.reshape(-1)[: small.size].reshape(small.shape)
    return lax.psum(small, ORDER)


def on_device(ids, targets, segments, table, table_m, table_v, blocks, left_stats, right_stats,
              left_root, right_root, gains, gains_m, gains_v):
    blk, shard = lax.axis_size("blk"), lax.axis_size("shard")
    section = lax.axis_index("section")
    blk_index, shard_index = lax.axis_index("blk"), lax.axis_index("shard")
    devices = 2 * blk * shard
    micro, _, tok_rows = ids.shape
    seq_len = segments.shape[2]
    all_tokens = micro * shard * seq_len
    tokens = all_tokens // devices
    seq_blocks = seq_len // tokens
    reach = pl.cdiv(seq_len // 2 - 1, tokens)
    vocab = table.shape[0]
    padded = pl.cdiv(vocab, 128) * 128
    own_blocks = blocks.shape[1]

    mine = my_block()
    slot = (blk_index * shard + shard_index) * 2 + section
    seg_own = lax.dynamic_slice_in_dim(segments[:, 0, :], blk_index * tok_rows, tok_rows, axis=1)
    packed = jnp.stack(
        [ids[:, 0, :], targets[:, 0, :, 0], targets[:, 0, :, 1], seg_own], axis=0
    ).reshape(4 * micro, tok_rows)
    shared = share_ids(packed, 8).reshape(blk, shard, 4, micro, tok_rows)
    shared = shared.transpose(2, 3, 1, 0, 4).reshape(4, devices, tokens)
    first_row = ((section * blk + blk_index) * shard + shard_index) * vocab
    placed = jnp.stack([shared.reshape(4, devices // 4, 4, tokens)[:3, :, i] for i in CORNER], axis=2)
    placed = placed.reshape(3, devices, tokens)
    local_ids, local_first, local_second = (placed[i] - first_row for i in range(3))

    def mark(values):
        return jnp.where((values >= 0) & (values < vocab), values, -1)

    local_ids, local_first, local_second = mark(local_ids), mark(local_first), mark(local_second)
    seg_index = jnp.maximum(mine - jnp.arange(reach + 1), 0)
    seg_rows = jnp.take(shared[3], seg_index, axis=0).astype(f32)[:, None, :]

    rows_low = blocks_to_rows(blocks[0].astype(bf16))
    table_low = jnp.pad(table.astype(bf16), ((0, padded - vocab), (0, 0)))
    gathered, looked = gather_and_lookup(rows_low, 0, local_ids, table_low)
    weights = jnp.stack([rows_to_quads(part, own_blocks) for part in gathered.reshape(
        2, blk * shard * rows_low.shape[0], QUAD)]) if own_blocks % 4 else gathered.reshape(
        2, QUADS, BS, QUAD)
    states = scatter_all(looked, 1).astype(f32)

    positions = (mine % seq_blocks) * tokens + jnp.arange(tokens, dtype=jnp.int32)
    cosine, sine = rope_tables(positions)
    rows_of_gain = [gains[i : i + 1] for i in range(5)]
    caches = []
    for l in range(2):
        a, q, k, v = qkv_forward(l, states, rows_of_gain[2 * l], cosine, sine, weights)
        total, accum, far_k, far_v = attend(q, k, v, seg_rows, reach, seq_blocks, 2)
        out, att, mixed, nm, gate, upper, hidden, normed_own = mlp_forward(
            l, l == 1, states, accum, total, rows_of_gain[2 * l + 1], rows_of_gain[4], weights
        )
        caches.append(
            (states, a, q, k, v, far_k, far_v, total, accum, (mixed, nm, gate, upper, hidden, att))
        )
        states = out
    normed = gather_all(normed_own, 3)
    top, spread_sum, expo, picks = vocab_stats(
        normed, table_low, local_first, local_second, vocab
    )
    log_total = share_stats(top, spread_sum, 4)
    inv_count = 1.0 / all_tokens
    grad_rows, head_term = vocab_grads(
        expo, normed, table_low, top, log_total, local_first, local_second, inv_count
    )
    own_log = lax.dynamic_index_in_dim(log_total, slot, 0, keepdims=False)
    loss_part = (1.0 + second_weight) * jnp.sum(own_log) - jnp.sum(picks)
    grad = scatter_all(grad_rows, 1)
    gain_grads = [None] * 5
    store = None
    for l in (1, 0):
        before, a, q, k, v, far_k, far_v, total, accum, cache = caches[l]
        store, grad_mixed, grad_att, gain_grads[2 * l + 1], final_row = mlp_backward(
            l, l == 1, grad, states, cache, rows_of_gain[2 * l + 1], rows_of_gain[4], weights, store
        )
        if l == 1:
            gain_grads[4] = final_row
        dq, dk, dv = attend_back(
            q, k, v, far_k, far_v, total, accum, grad_att, seg_rows, reach, seq_blocks, 5
        )
        store, grad, grad_low, gain_grads[2 * l] = qkv_backward(
            l, dq, dk, dv, a, before, grad_mixed, rows_of_gain[2 * l], cosine, sine, weights, store
        )
    sends = store
    if own_blocks % 4:
        sends = jnp.stack([quads_to_rows(store[l], own_blocks) for l in range(2)])
    sends = sends.reshape(devices, rows_low.shape[0], QUAD)
    grad_embed = gather_all(grad_low, 3)
    block_rows, table_own = scatter_and_spread(sends, 6, local_ids, grad_embed, head_term)
    table_own = table_own[:vocab]
    square_rows = block_rows.astype(f32)
    square_sum = jnp.sum(table_own * table_own) + jnp.sum(square_rows * square_rows)
    small = jnp.concatenate(
        gain_grads
        + [jnp.full((1, D), square_sum), jnp.full((1, D), loss_part), jnp.zeros((1, D), f32)]
    )
    summed = share_sum(small, 7)
    gain_grad = summed[:5]
    clip_norm = jnp.sqrt(summed[5, 0] + jnp.sum(gain_grad * gain_grad))
    factor = clip_bound / jnp.maximum(clip_norm, clip_bound)
    loss = summed[6, 0] * inv_count
    update = shampoo if own_blocks % 12 == 0 else shampoo_plain
    blocks_new, blocks_low, left_new, right_new = update(
        factor, block_rows, blocks[0], left_stats[0], right_stats[0], left_root[0], right_root[0]
    )
    table_new, table_m_new, table_v_new = adam_step(
        table, table_m, table_v, table_own * factor, weight_decay
    )
    gains_new, gains_m_new, gains_v_new = adam_step(
        gains, gains_m, gains_v, gain_grad * factor, 0.0
    )
    return (
        loss, clip_norm, table_new, table_m_new, table_v_new, table_new.astype(bf16),
        blocks_new[None], blocks_low[None], left_new[None], right_new[None],
        gains_new, gains_m_new, gains_v_new,
    )


def solution(mesh):
    rows = P(("section", "blk", "shard"), None)
    square = P("section", ("blk", "shard"), None, None)
    return jax.shard_map(
        on_device,
        mesh=mesh,
        in_specs=(
            P(None, "shard", "blk"),
            P(None, "shard", "blk", None),
            P(None, "shard", None),
            rows, rows, rows,
            square, square, square, square, square,
            P(), P(), P(),
        ),
        out_specs=(
            P(), P(),
            rows, rows, rows, rows,
            square, square, square, square,
            P(), P(), P(),
        ),
        check_vma=False,
    )
```
